32 devices in a mesh: dom: 32 (over z, y, x, core).
Axes of the slice: x: 2, y: 2, z: 4, core: 2. Of those that a mesh axis runs over, the one named last changes fastest.
Arguments:
- particles: bfloat16 [1024, 2, 7488], P('dom'), may hold values from -6 to 6
- references: bfloat16 [32, 2, 7488], P('dom'), may hold values from -6 to 6
- assignment: int32 [1024, 1], P('dom'), may hold values from 0 to 31
- orientation: int32 [1024], P('dom'), may hold values from 0 to 35
- tilt_range: int32 [2, 1024], P(None, 'dom'), may hold values from 0 to 20
Outputs:
- scores: float32 [1024, 32], P('dom')
- class_means: float32 [32, 2, 7488], P('dom')
- class_load: float32 [32], replicated
The draws below stay inside these ranges and needn't reach their ends.
Inputs may be any that keep to these rules, and one draw needn't show every extreme that they name: `assignment`: every class has at least one particle.
All inputs are finite; a program needn't handle non-finite values.
Results may differ from the reference program's by a relative error of at most 0.0035.
Values may be sent and summed in bfloat16 or wider, within the bound.
No kernel may reach another device: no remote copies, remote signals or barrier semaphores. Data moves between devices by JAX's collectives and lax.ppermute only.
A program may use at most 128 MiB of HBM per device.

```python
import math
import jax
import jax.numpy as jnp
from jax import lax

GRID = 24
ORIENTS = 36
TILT_BINS = 21
PART_DEV = 32
CLASSES = 32
COEF = 7488
PARTICLES = 1024
N_DOM = 32


def with_ends(drawn, own_key, least, largest):
    place = [jax.random.randint(jax.random.fold_in(own_key, axis), (), 0, length) for axis, length in enumerate(drawn.shape)]
    widest = drawn.shape.index(max(drawn.shape))
    neighbour = place[:widest] + [(place[widest] + 1) % drawn.shape[widest]] + place[widest + 1:]
    return drawn.at[tuple(place)].set(least).at[tuple(neighbour)].set(largest)


def level_of(key, dims, cuts, low, largest):
    loudness = 1.0
    for axis_at, parts in cuts:
        draws = jax.random.uniform(jax.random.fold_in(jax.random.fold_in(key, 6), axis_at), (parts,), jnp.float32, low / len(cuts), largest / len(cuts))
        loudness = loudness * jnp.repeat(jnp.exp(draws), dims[axis_at] // parts).reshape((-1,) + (1,) * (len(dims) - 1 - axis_at))
    return loudness


def picks_of(rng, rows, number_of, top, lift):
    sequence = jax.random.permutation(jax.random.fold_in(rng, 1), number_of)
    boost = sequence
    for power in range(3):
        boost = boost * boost // number_of
    boost = boost * lift // number_of
    chance = jax.random.randint(jax.random.fold_in(rng, 2), (rows, number_of), 0, 4096) + boost
    holders = jax.random.permutation(jax.random.fold_in(rng, 3), rows)[jnp.arange(number_of) % rows]
    chance = jnp.where(jnp.arange(rows)[:, None] == holders[None, :], 1 << 14, chance)
    priority = chance * number_of + jnp.arange(number_of)
    return lax.top_k(priority.astype(jnp.int32), top)[1].astype(jnp.int32)


def noise(rng, shape, spread, most, pieces=(), kind=jnp.bfloat16):
    array = jax.random.normal(rng, shape, jnp.float32) * spread
    if len(pieces) > 0:
        array = level_of(rng, shape, pieces, -0.22, 0.18) * array
    return jnp.clip(array, min=-most, max=most).astype(kind)


def setup_inputs(seed: int = 0) -> dict:
    keys = jax.random.split(jax.random.key(seed), 6)
    return {
        "particles": noise(keys[0], (PARTICLES, 2, COEF), 1.0, 6.0, ((0, 32),)),
        "references": noise(keys[1], (CLASSES, 2, COEF), 1.0, 6.0, ((0, 32),)),
        "assignment": picks_of(keys[2], PARTICLES, CLASSES, 1, 256),
        "orientation": with_ends(jax.random.randint(keys[3], (PARTICLES,), 0, ORIENTS), jax.random.fold_in(keys[3], 1), 0, ORIENTS - 1).astype(jnp.int32),
        "tilt_range": with_ends(jax.random.randint(keys[4], (2, PARTICLES), 0, TILT_BINS), jax.random.fold_in(keys[4], 1), 0, TILT_BINS - 1).astype(jnp.int32),
    }


EPS = 1e-06
GAIN = 6.0
TAU = 0.5

def tables():
    index = jnp.arange(COEF, dtype=jnp.int32)
    plane = index // (GRID * GRID)
    rest = index % (GRID * GRID)
    col_x = rest // GRID
    col_z = rest % GRID
    freq_x = ((col_x + GRID // 2) % GRID - GRID // 2).astype(jnp.float32)
    freq_y = plane.astype(jnp.float32)
    freq_z = ((col_z + GRID // 2) % GRID - GRID // 2).astype(jnp.float32)
    return (freq_x, freq_y, freq_z)

def wedge_weights(orient, low_bin, high_bin):
    freq_x, freq_y, freq_z = tables()
    angle = orient.astype(jnp.float32) * (2.0 * math.pi / ORIENTS)
    along = -freq_x[None, :] * jnp.sin(angle)[:, None] + freq_y[None, :] * jnp.cos(angle)[:, None]
    radius = along * along + freq_z[None, :] * freq_z[None, :] + 1.0
    cos_two = (along * along - freq_z[None, :] * freq_z[None, :]) / radius
    sin_two = -2.0 * along * freq_z[None, :] / radius
    low = -(40.0 + 1.5 * low_bin.astype(jnp.float32)) * (math.pi / 180.0)
    high = (40.0 + 1.5 * high_bin.astype(jnp.float32)) * (math.pi / 180.0)
    centre = (low + high)[:, None]
    width = (high - low)[:, None]
    return jax.nn.sigmoid(GAIN * (cos_two * jnp.cos(centre) + sin_two * jnp.sin(centre) - jnp.cos(width)))

def reference(particles, references, assignment, orientation, tilt_range):
    ref32 = references.astype(jnp.float32)
    ref_power = (ref32[:, 0] * ref32[:, 0] + ref32[:, 1] * ref32[:, 1]).astype(jnp.bfloat16)
    ref_flat = references.reshape(CLASSES, 2 * COEF)
    part_blocks = particles.reshape(N_DOM, PART_DEV, 2, COEF)
    cls_blocks = assignment.reshape(N_DOM, PART_DEV)
    ori_blocks = orientation.reshape(N_DOM, PART_DEV)
    tilt_blocks = tilt_range.reshape(2, N_DOM, PART_DEV).transpose(1, 0, 2)
    class_ids = jnp.arange(CLASSES, dtype=jnp.int32)

    def step(carry, item):
        numer, denom, counts, totals = carry
        part, cls, ori, tilt = item
        wedge = wedge_weights(ori, tilt[0], tilt[1])
        pf = part.astype(jnp.float32)
        weighted = (wedge[:, None, :] * pf).astype(jnp.bfloat16)
        flat = weighted.reshape(PART_DEV, 2 * COEF)
        wedge_sq = (wedge * wedge).astype(jnp.bfloat16)
        wedge_low = wedge.astype(jnp.bfloat16)
        power = lax.optimization_barrier(jnp.sum(wedge * (pf[:, 0] * pf[:, 0] + pf[:, 1] * pf[:, 1]), axis=1))
        intersection = jnp.dot(flat, ref_flat.T, preferred_element_type=jnp.float32)
        energy = jnp.dot(wedge_low, ref_power.T, preferred_element_type=jnp.float32)
        scores = intersection / (math.sqrt(COEF) * jnp.sqrt((energy / COEF + EPS) * (power[:, None] / COEF + EPS)))
        onehot = (class_ids[:, None] == cls[None, :]).astype(jnp.bfloat16)
        numer = numer + jnp.dot(onehot, flat, preferred_element_type=jnp.float32)
        denom = denom + jnp.dot(onehot, wedge_sq, preferred_element_type=jnp.float32)
        onehot32 = onehot.astype(jnp.float32)
        counts = counts + lax.optimization_barrier(jnp.sum(onehot32, axis=1))
        totals = totals + jnp.dot(onehot32, lax.optimization_barrier(jnp.sum(wedge, axis=1)), precision=lax.Precision.HIGHEST)
        return ((numer, denom, counts, totals), scores)
    start = (jnp.zeros((CLASSES, 2 * COEF), jnp.float32), jnp.zeros((CLASSES, COEF), jnp.float32), jnp.zeros((CLASSES,), jnp.float32), jnp.zeros((CLASSES,), jnp.float32))
    (numer, denom, counts, totals), scores = lax.scan(step, start, (part_blocks, cls_blocks, ori_blocks, tilt_blocks))
    scores = scores.reshape(PARTICLES, CLASSES)
    bottom = denom + TAU * (totals[:, None] / COEF + 1.0)
    class_means = numer.reshape(CLASSES, 2, COEF) / bottom[:, None, :]
    class_load = counts * CLASSES / PARTICLES
    return (scores, class_means, class_load)
```

```python
import math

import jax
import jax.numpy as jnp
from jax import lax
from jax.sharding import PartitionSpec as P

GRID = 24
ORIENTS = 36
COEF = 7488


EPS = 1e-06
GAIN = 6.0
TAU = 0.5
member_rows = 256


def tables():
    index = jnp.arange(COEF, dtype=jnp.int32)
    plane = index // (GRID * GRID)
    rest = index % (GRID * GRID)
    col_x = rest // GRID
    col_z = rest % GRID
    freq_x = ((col_x + GRID // 2) % GRID - GRID // 2).astype(jnp.float32)
    freq_y = plane.astype(jnp.float32)
    freq_z = ((col_z + GRID // 2) % GRID - GRID // 2).astype(jnp.float32)
    return (freq_x, freq_y, freq_z)


def wedge_weights(orient, low_bin, high_bin):
    freq_x, freq_y, freq_z = tables()
    angle = orient.astype(jnp.float32) * (2.0 * math.pi / ORIENTS)
    along = -freq_x[None, :] * jnp.sin(angle)[:, None] + freq_y[None, :] * jnp.cos(angle)[:, None]
    radius = along * along + freq_z[None, :] * freq_z[None, :] + 1.0
    cos_two = (along * along - freq_z[None, :] * freq_z[None, :]) / radius
    sin_two = -2.0 * along * freq_z[None, :] / radius
    low = -(40.0 + 1.5 * low_bin.astype(jnp.float32)) * (math.pi / 180.0)
    high = (40.0 + 1.5 * high_bin.astype(jnp.float32)) * (math.pi / 180.0)
    centre = (low + high)[:, None]
    width = (high - low)[:, None]
    return jax.nn.sigmoid(
        GAIN * (cos_two * jnp.cos(centre) + sin_two * jnp.sin(centre) - jnp.cos(width))
    )


def body(particles, references, assignment, orientation, tilt_range):
    part_rows = particles.shape[0]
    coef = particles.shape[2]
    owned = references.shape[0]
    devices = lax.axis_size("dom")
    chips = devices // 2
    classes = owned * devices
    total = part_rows * devices
    assert owned == 1 and classes <= 256 and (4 * part_rows) % 2 == 0
    me = lax.axis_index("dom")
    core = me % 2
    groups = [[2 * q + c for q in range(chips)] for c in range(2)]
    swap = [(d, d ^ 1) for d in range(devices)]

    cls = assignment[:, 0]
    labels = jnp.stack([cls, orientation, tilt_range[0], tilt_range[1]])
    tail = labels.astype(jnp.bfloat16).reshape(1, 2, 2 * part_rows)
    packet = jnp.concatenate([references, tail], axis=2)
    packet = jnp.broadcast_to(packet, (chips, 2, coef + 2 * part_rows))
    same = lax.all_to_all(packet, "dom", 0, 0, axis_index_groups=groups, tiled=True)

    wedge = wedge_weights(orientation, tilt_range[0], tilt_range[1])
    pf = particles.astype(jnp.float32)
    weighted = (wedge[:, None, :] * pf).astype(jnp.bfloat16)
    flat = weighted.reshape(part_rows, 2 * coef)
    wedge_low = wedge.astype(jnp.bfloat16)
    power = jnp.sum(wedge * (pf[:, 0] * pf[:, 0] + pf[:, 1] * pf[:, 1]), axis=1)

    q_ids = lax.iota(jnp.int32, chips)

    def sums(parity):
        onehot = ((2 * q_ids + parity)[:, None] == cls[None, :]).astype(jnp.bfloat16)
        return jnp.dot(onehot, flat, preferred_element_type=jnp.float32)

    got = lax.ppermute(sums(1 - core), "dom", swap)
    chip_sum = (sums(core) + got).astype(jnp.bfloat16)
    arrived = lax.all_to_all(chip_sum, "dom", 0, 0, axis_index_groups=groups, tiled=True)

    other = lax.ppermute(same, "dom", swap)

    def score_part(block):
        piece = block[:, :, :coef]
        p32 = piece.astype(jnp.float32)
        ref_power = (p32[:, 0] * p32[:, 0] + p32[:, 1] * p32[:, 1]).astype(jnp.bfloat16)
        intersection = lax.dot_general(
            flat,
            piece.reshape(chips, 2 * coef),
            (((1,), (1,)), ((), ())),
            preferred_element_type=jnp.float32,
        )
        energy = lax.dot_general(
            wedge_low, ref_power, (((1,), (1,)), ((), ())), preferred_element_type=jnp.float32
        )
        return intersection / (
            math.sqrt(coef) * jnp.sqrt((energy / coef + EPS) * (power[:, None] / coef + EPS))
        )

    mine, theirs = score_part(same), score_part(other)
    scores = jnp.where(
        core == 0, jnp.stack([mine, theirs], axis=2), jnp.stack([theirs, mine], axis=2)
    ).reshape(part_rows, classes)

    every = jnp.concatenate([same[:, :, coef:], other[:, :, coef:]]).reshape(devices, 4, part_rows)
    every = every.transpose(1, 0, 2).reshape(4, total).astype(jnp.int32)
    class_ids = jnp.arange(classes, dtype=jnp.int32)
    counts = jnp.sum((class_ids[:, None] == every[0][None, :]).astype(jnp.float32), axis=1)
    chosen = every[0] == me
    members = jnp.nonzero(chosen, size=total + member_rows, fill_value=0)[0].astype(jnp.int32)
    members_count = jnp.sum(chosen.astype(jnp.int32))
    block_count = (members_count + member_rows - 1) // member_rows

    def member_block(block, acc):
        square_sum, wedge_sum = acc
        first = (block * member_rows).astype(jnp.int32)
        picked = lax.dynamic_slice_in_dim(members, first, member_rows, 0)
        valid = (first + lax.iota(jnp.int32, member_rows) < members_count).astype(jnp.float32)
        member_wedge = wedge_weights(every[1][picked], every[2][picked], every[3][picked])
        squares = (member_wedge * member_wedge).astype(jnp.bfloat16).astype(jnp.float32)
        square_sum = square_sum + jnp.sum(valid[:, None] * squares, axis=0)
        wedge_sum = wedge_sum + jnp.sum(valid * jnp.sum(member_wedge, axis=1))
        return (square_sum, wedge_sum)

    square_sum, wedge_sum = lax.fori_loop(
        0, block_count, member_block, (jnp.zeros((coef,), jnp.float32), jnp.zeros((), jnp.float32))
    )
    numer = jnp.sum(arrived.astype(jnp.float32), axis=0).reshape(owned, 2, coef)
    bottom = square_sum + TAU * (wedge_sum / coef + 1.0)
    class_means = numer / bottom[None, None, :]
    class_load = counts * classes / total
    return (scores, class_means, class_load)


def solution(mesh):
    in_specs = (
        P("dom", None, None),
        P("dom", None, None),
        P("dom", None),
        P("dom"),
        P(None, "dom"),
    )
    out_specs = (P("dom", None), P("dom", None, None), P())
    return jax.shard_map(body, mesh=mesh, in_specs=in_specs, out_specs=out_specs, check_vma=False)
```

```python
import functools
import math

import jax
import jax.numpy as jnp
from jax import lax
from jax.experimental import pallas as pl
from jax.experimental.pallas import tpu as pltpu
from jax.sharding import PartitionSpec as P


GRID = 24
ORIENTS = 36

EPS = 1e-06
GAIN = 6.0
TAU = 0.5
LOG2E = math.log2(math.e)
LANES = 128
STEP = 256
CHUNK = 512
GROUP = 128
FAR = 4
VMEM = pltpu.VMEM
f32 = jnp.float32
bf16 = jnp.bfloat16
i32 = jnp.int32


def iota(shape, axis):
    return lax.broadcasted_iota(i32, shape, axis)


def dot(a, b):
    return jnp.dot(a, b, preferred_element_type=f32)


def dot_nt(a, b):
    return lax.dot_general(a, b, (((1,), (1,)), ((), ())), preferred_element_type=f32)


def freqs(index):
    plane = jnp.floor((index + 0.5) * (1.0 / (GRID * GRID)))
    rest = index - plane * (GRID * GRID)
    col_x = jnp.floor((rest + 0.5) * (1.0 / GRID))
    col_z = rest - col_x * GRID
    half = GRID // 2
    freq_x = jnp.where(col_x < half, col_x, col_x - GRID)
    freq_z = jnp.where(col_z < half, col_z, col_z - GRID)
    return freq_x, plane, freq_z


def wedge_of(freq_x, freq_y, freq_z, sin_a, cos_a, cos_c, sin_c, cos_w):
    along = freq_y * cos_a - freq_x * sin_a
    sq = along * along
    zsq = freq_z * freq_z
    inverse = 1.0 / (sq + (zsq + 1.0))
    power = (cos_c * (sq - zsq) + sin_c * (along * freq_z)) * inverse + cos_w
    return 1.0 / (1.0 + jnp.exp2(power))


def by_lane(values, width):
    lane = iota((1, width), 1)
    row = jnp.zeros((1, width), f32)
    for i, value in enumerate(values):
        row = jnp.where(lane == i, f32(value), row)
    return row


def turns(orient, low_bin, high_bin, width):
    quarter = 0.5 * math.pi
    bin_ = 1.5 * math.pi / 180.0
    wide = 80.0 * math.pi / 180.0
    scale = GAIN * LOG2E
    turn = (
        orient * by_lane([2.0 * math.pi / ORIENTS] * 2, width)
        + low_bin * by_lane([0.0, 0.0, -bin_, -bin_, bin_], width)
        + high_bin * by_lane([0.0, 0.0, bin_, bin_, bin_], width)
        + by_lane([0.0, quarter, quarter, 0.0, quarter + wide], width)
    )
    return jnp.sin(turn) * by_lane([1.0, 1.0, -scale, 2.0 * scale, scale], width)


def to_column(row):
    size = row.shape[1]
    same = iota((size, size), 0) == iota((size, size), 1)
    return jnp.sum(jnp.where(same, row, 0.0), axis=1, keepdims=True)


def pack_kernel(padded, ref_ref, cls_ref, orient_ref, tilt_ref, packet_ref, pack, sems):
    coef = ref_ref.shape[2]
    parts = orient_ref.shape[0]
    cls = cls_ref[...].reshape(1, parts)
    orient = orient_ref[...].reshape(1, parts)
    first = jnp.where(iota((2, parts), 0) == 0, cls, orient).astype(f32).astype(bf16)
    second = tilt_ref[...].astype(f32).astype(bf16)
    source, lane = iota((parts, LANES), 0), iota((parts, LANES), 1)
    labels = dot(first, (lane == source).astype(bf16)) + dot(
        second, (lane == source + parts).astype(bf16)
    )
    pack[:, 0:coef] = ref_ref[0]
    pack[:, padded : padded + LANES] = labels.astype(bf16)
    copies = [
        pltpu.make_async_copy(pack, packet_ref.at[q], sems.at[q])
        for q in range(packet_ref.shape[0])
    ]
    for copy in copies:
        copy.start()
    for copy in copies:
        copy.wait()


def pre_kernel(
    coef, chips, rows, half,
    x_ref, cls_ref, orient_ref, tilt_ref,
    keep_ref, send_ref, weighted_ref, low_ref, power_ref,
):
    parts = x_ref.shape[0]
    padded = low_ref.shape[1]
    full = coef // STEP * STEP
    cls = cls_ref[...].reshape(1, parts)
    orient = orient_ref[...].reshape(1, parts)
    core = lax.axis_index("dom") % 2
    order = iota((2 * chips, parts), 0)
    order = jnp.where(order < chips, 2 * order + core, 2 * (order - chips) + 1 - core)
    hot = (order == cls).astype(bf16)
    turn = turns(
        to_column(orient.astype(f32)),
        to_column(tilt_ref[0:1, :].astype(f32)),
        to_column(tilt_ref[1:2, :].astype(f32)),
        LANES,
    )
    factors = [turn[:, i : i + 1] for i in range(5)]
    out_row, in_row = iota((2 * parts, 2 * parts), 0), iota((2 * parts, 2 * parts), 1)
    wanted = jnp.where(out_row < parts, 2 * out_row, 2 * (out_row - parts) + 1)
    split = (in_row == wanted).astype(bf16)

    def block(x, start, width, valid):
        both = dot(split, x.reshape(2 * parts, x.shape[2]))
        if valid < width:
            both = jnp.concatenate([both, jnp.zeros((2 * parts, width - valid), f32)], axis=1)
        real, imag = both[:parts], both[parts:]
        index = (iota((1, width), 1) + start).astype(f32)
        wedge = wedge_of(*freqs(index), *factors)
        if valid < width:
            wedge = jnp.where(index < coef, wedge, 0.0)
        cols = pl.ds(start, width)
        low_ref[:, cols] = wedge.astype(bf16)
        energy = wedge * (real * real + imag * imag)
        total = energy[:, :LANES]
        for j in range(1, width // LANES):
            total = total + energy[:, j * LANES : (j + 1) * LANES]
        power_ref[...] += total
        tile = start // LANES
        for part, value in enumerate((real, imag)):
            value = (wedge * value).astype(bf16)
            weighted_ref[part * parts : (part + 1) * parts, cols] = value
            summed = dot(hot, value)
            for j in range(width // LANES):
                for q in range(0, chips, 8):
                    place = pl.ds(q * rows + part * half + tile + j, 8, stride=rows)
                    lanes = slice(j * LANES, (j + 1) * LANES)
                    keep_ref[place, :] = summed[q : q + 8, lanes]
                    send_ref[place, :] = summed[chips + q : chips + q + 8, lanes]

    power_ref[...] = jnp.zeros_like(power_ref)

    def step(s, carry):
        start = pl.multiple_of(s * STEP, STEP)
        block(x_ref[:, :, pl.ds(start, STEP)], start, STEP, STEP)
        return carry

    lax.fori_loop(0, full // STEP, step, 0)
    block(x_ref[:, :, full:coef], full, padded - full, coef - full)


def add_kernel(chips, rows, room, keep_ref, got_ref, out_ref):
    for q in range(chips):
        place = pl.ds(q * rows, room)
        out_ref[q] = (keep_ref[place, :] + got_ref[place, :]).astype(bf16)


def table_kernel(table_ref):
    for t in range(table_ref.shape[2] // LANES):
        index = (iota((8, LANES), 1) + t * LANES).astype(f32)
        for i, row in enumerate(freqs(index)):
            table_ref[i, :, t * LANES : (t + 1) * LANES] = row


def post_kernel(
    coef, same_ref, other_ref, weighted_ref, low_ref, power_ref, table,
    score_ref, load_ref, bottom_ref,
    squares, listed,
):
    chips = same_ref.shape[0]
    parts, padded = low_ref.shape
    devices = 2 * chips
    per_far = chips // FAR
    classes = score_ref.shape[1]
    tiles = padded // LANES
    me = lax.axis_index("dom")
    core = me % 2

    def picker(parity):
        out_row, in_row = iota((2 * devices, 2 * chips), 0), iota((2 * devices, 2 * chips), 1)
        part = (out_row >= devices).astype(i32)
        device = out_row - part * devices
        chip = device // 2
        near = (chip % per_far) ^ (me // 2 % per_far)
        place = near * FAR + chip // per_far
        return (in_row == 2 * place + part) & (device % 2 == parity)

    pick_a, pick_b = picker(core).astype(bf16), picker(1 - core).astype(bf16)

    def rows_of(start, width):
        cols = pl.ds(start, width)
        a = same_ref[:, :, cols].reshape(2 * chips, width)
        b = other_ref[:, :, cols].reshape(2 * chips, width)
        return dot(pick_a, a) + dot(pick_b, b)

    labels = rows_of(padded, LANES)
    cls, orient = labels[:devices, :parts], labels[devices:, :parts]
    low_bin, high_bin = labels[:devices, parts : 2 * parts], labels[devices:, parts : 2 * parts]
    class_col = iota((classes, parts), 0).astype(f32)
    tally = jnp.zeros((classes, parts), f32)
    for r in range(devices):
        tally = tally + jnp.where(cls[r : r + 1] == class_col, 1.0, 0.0)
    tally = jnp.sum(tally, axis=1, keepdims=True)
    diagonal = iota((classes, classes), 0) == iota((classes, classes), 1)
    counts = jnp.sum(jnp.where(diagonal, tally, 0.0), axis=0, keepdims=True)
    load_ref[...] = counts * (classes / (devices * parts))

    chosen = cls == me.astype(f32)
    mask = chosen.astype(bf16)
    before = (iota((parts, parts), 0) < iota((parts, parts), 1)).astype(bf16)
    above = (iota((devices, devices), 0) > iota((devices, devices), 1)).astype(bf16)
    in_row = dot(mask, jnp.ones((parts, parts), bf16))
    rank = dot(mask, before) + dot(above, in_row.astype(bf16))
    rank = jnp.where(chosen, rank, -1.0)
    count = jnp.sum(jnp.where(chosen, 1.0, 0.0)).astype(i32)

    squares[...] = jnp.zeros_like(squares)

    def group(g, total):
        base = (g * GROUP).astype(f32)
        slot = iota((GROUP, parts), 0).astype(f32) + base
        values = [jnp.zeros((GROUP, 1), f32)] * 3
        columns = jnp.zeros((GROUP, 8), f32)
        pick = iota((8, parts), 0)
        for r in range(devices):
            hit = (rank[r : r + 1] == slot).astype(bf16)
            row = jnp.where(pick == 0, orient[r : r + 1], jnp.where(pick == 1, low_bin[r : r + 1], high_bin[r : r + 1]))
            columns = columns + dot_nt(hit, row.astype(bf16))
        turn = turns(columns[:, 0:1], columns[:, 1:2], columns[:, 2:3], 8)
        empty = iota((GROUP, 8), 0) + g * GROUP >= count
        listed[...] = jnp.where(empty & (iota((GROUP, 8), 1) == 4), 100.0, turn)
        left = jnp.minimum(count - g * GROUP, GROUP)

        def eight(e, total):
            params = listed[pl.ds(pl.multiple_of(e * 8, 8), 8), :]
            factors = [jnp.broadcast_to(params[:, i : i + 1], (8, LANES)) for i in range(5)]
            for t in range(tiles):
                cols = slice(t * LANES, (t + 1) * LANES)
                wedge = wedge_of(table[0, :, cols], table[1, :, cols], table[2, :, cols], *factors)
                squares[:, cols] += (wedge * wedge).astype(bf16).astype(f32)
                if (t + 1) * LANES > coef:
                    wedge = jnp.where(iota((8, LANES), 1) < coef - t * LANES, wedge, 0.0)
                total = total + wedge
            return total

        return lax.fori_loop(0, (left + 7) // 8, eight, total)

    total = lax.fori_loop(0, (count + GROUP - 1) // GROUP, group, jnp.zeros((8, LANES), f32))
    extra = TAU * (jnp.sum(total, keepdims=True) * (1.0 / coef) + 1.0)
    for t in range(tiles):
        cols = slice(t * LANES, (t + 1) * LANES)
        bottom_ref[t : t + 1, :] = jnp.sum(squares[:, cols], axis=0, keepdims=True) + extra

    intersection = jnp.zeros((parts, classes), f32)
    energy = jnp.zeros((parts, classes), f32)
    for start in range(0, padded, CHUNK):
        width = min(CHUNK, padded - start)
        cols = slice(start, start + width)
        both = rows_of(start, width)
        real, imag = both[:devices], both[devices:]
        ref_power = (real * real + imag * imag).astype(bf16)
        intersection = intersection + dot_nt(weighted_ref[:parts, cols], real.astype(bf16))
        intersection = intersection + dot_nt(weighted_ref[parts:, cols], imag.astype(bf16))
        energy = energy + dot_nt(low_ref[:, cols], ref_power)
    power = jnp.sum(power_ref[...], axis=1, keepdims=True)
    score_ref[...] = intersection / (
        math.sqrt(coef) * jnp.sqrt((energy / coef + EPS) * (power / coef + EPS))
    )


def final_kernel(coef, half, arrived_ref, bottom_ref, out_ref, ratio):
    tiles = -(-coef // LANES)
    total = arrived_ref[0].astype(f32)
    for q in range(1, arrived_ref.shape[0]):
        total = total + arrived_ref[q].astype(f32)
    bottom = bottom_ref[...]
    ratio[0:half, :] = total[0:half] / bottom[0:half]
    ratio[half : 2 * half, :] = total[half : 2 * half] / bottom[0:half]
    for t in range(tiles):
        width = min(LANES, coef - t * LANES)
        pair = ratio[pl.ds(t, 2, stride=half), :]
        out_ref[0, :, pl.ds(t * LANES, width)] = pair[:, :width]


def limit(*arrays):
    size = sum(math.prod(a.shape) * max(2, jnp.dtype(a.dtype).itemsize) for a in arrays)
    return pltpu.CompilerParams(vmem_limit_bytes=(4 << 20) + size)


def body(particles, references, assignment, orientation, tilt_range):
    part_rows = particles.shape[0]
    coef = particles.shape[2]
    owned = references.shape[0]
    devices = lax.axis_size("dom")
    chips = devices // 2
    classes = owned * devices
    assert owned == 1 and classes <= 256 and chips % 8 == 0 and chips & (chips - 1) == 0 and 2 * part_rows <= LANES
    groups = [[2 * q + c for q in range(chips)] for c in range(2)]
    near = devices // FAR
    far = [[d + near * q for q in range(FAR)] for d in range(near)]
    swap = [(d, d ^ 1) for d in range(devices)]
    tiles = -(-coef // LANES)
    half = -(-tiles // 4) * 4
    room = 2 * half
    rows = room + 1
    padded = tiles * LANES
    wide = padded + LANES
    assert padded - coef // STEP * STEP <= LANES
    shape = jax.ShapeDtypeStruct
    hbm = pl.BlockSpec(memory_space=pltpu.HBM)
    vmem = pl.BlockSpec(memory_space=VMEM)

    cls = assignment.reshape(part_rows)
    packet = pl.pallas_call(
        functools.partial(pack_kernel, padded),
        out_shape=shape((FAR, 2, wide), bf16),
        in_specs=[vmem] * 4,
        out_specs=hbm,
        scratch_shapes=[VMEM((2, wide), bf16), pltpu.SemaphoreType.DMA((FAR,))],
        compiler_params=pltpu.CompilerParams(vmem_limit_bytes=4 << 20),
        name="pack",
    )(references, cls, orientation, tilt_range)

    same = lax.all_to_all(packet, "dom", 0, 0, axis_index_groups=far, tiled=True)
    outs = (
        shape((chips * rows, LANES), f32),
        shape((chips * rows, LANES), f32),
        shape((2 * part_rows, padded), bf16),
        shape((part_rows, padded), bf16),
        shape((part_rows, LANES), f32),
    )
    keep, send, weighted, low, power = pl.pallas_call(
        functools.partial(pre_kernel, coef, chips, rows, half),
        out_shape=outs,
        in_specs=[vmem, vmem, vmem, vmem],
        out_specs=(vmem, vmem, vmem, vmem, vmem),
        compiler_params=limit(*outs, particles),
        name="pre",
    )(particles, cls, orientation, tilt_range)
    got = lax.ppermute(send, "dom", swap)
    chip_sum = pl.pallas_call(
        functools.partial(add_kernel, chips, rows, room),
        out_shape=shape((chips, room, LANES), bf16),
        in_specs=[vmem, vmem],
        out_specs=vmem,
        compiler_params=limit(keep, got, keep),
        name="add",
    )(keep, got)
    arrived = lax.all_to_all(chip_sum, "dom", 0, 0, axis_index_groups=groups, tiled=True)
    table = pl.pallas_call(
        table_kernel,
        out_shape=shape((3, 8, padded), f32),
        out_specs=vmem,
        compiler_params=pltpu.CompilerParams(vmem_limit_bytes=4 << 20),
        name="table",
    )()
    bit = 1
    while bit < chips // FAR:
        swapped = lax.ppermute(same, "dom", [(d, d ^ (2 * bit)) for d in range(devices)])
        same = jnp.concatenate([same, swapped])
        bit *= 2
    other = lax.ppermute(same, "dom", swap)

    outs = (
        shape((part_rows, classes), f32),
        shape((1, classes), f32),
        shape((-(-tiles // 8) * 8, LANES), f32),
    )
    scores, load, bottom = pl.pallas_call(
        functools.partial(post_kernel, coef),
        out_shape=outs,
        in_specs=[vmem] * 6,
        out_specs=(vmem, vmem, vmem),
        scratch_shapes=[
            VMEM((8, padded), f32),
            VMEM((GROUP, 8), f32),
        ],
        compiler_params=limit(same, other, weighted, low, table, *outs),
        name="post",
    )(same, other, weighted, low, power, table)

    class_means = pl.pallas_call(
        functools.partial(final_kernel, coef, half),
        out_shape=shape((owned, 2, coef), f32),
        in_specs=[vmem, vmem],
        out_specs=vmem,
        scratch_shapes=[VMEM((room, LANES), f32)],
        compiler_params=limit(arrived),
        name="means",
    )(arrived, bottom)
    return (scores, class_means, load.reshape(classes))


def solution(mesh):
    in_specs = (
        P("dom", None, None),
        P("dom", None, None),
        P("dom", None),
        P("dom"),
        P(None, "dom"),
    )
    out_specs = (P("dom", None), P("dom", None, None), P())
    return jax.shard_map(body, mesh=mesh, in_specs=in_specs, out_specs=out_specs, check_vma=False)
```

```python
import functools
import math

import jax
import jax.numpy as jnp
from jax import lax
from jax.experimental import pallas as pl
from jax.experimental.pallas import tpu as pltpu
from jax.sharding import PartitionSpec as P


GRID = 24
ORIENTS = 36

EPS = 1e-06
GAIN = 6.0
TAU = 0.5
LOG2E = math.log2(math.e)
LANES = 128
STEP = 512
CHUNK = 512
GROUP = 128
FAR = 4
VMEM = pltpu.VMEM
f32 = jnp.float32
bf16 = jnp.bfloat16
i32 = jnp.int32


def iota(shape, axis):
    return lax.broadcasted_iota(i32, shape, axis)


def dot(a, b):
    return jnp.dot(a, b, preferred_element_type=f32)


def dot_nt(a, b):
    return lax.dot_general(a, b, (((1,), (1,)), ((), ())), preferred_element_type=f32)


def freqs(index):
    plane = jnp.floor((index + 0.5) * (1.0 / (GRID * GRID)))
    rest = index - plane * (GRID * GRID)
    col_x = jnp.floor((rest + 0.5) * (1.0 / GRID))
    col_z = rest - col_x * GRID
    half = GRID // 2
    freq_x = jnp.where(col_x < half, col_x, col_x - GRID)
    freq_z = jnp.where(col_z < half, col_z, col_z - GRID)
    return freq_x, plane, freq_z


def wedge_of(freq_x, freq_y, freq_z, sin_a, cos_a, cos_c, sin_c, cos_w):
    along = freq_y * cos_a - freq_x * sin_a
    sq = along * along
    zsq = freq_z * freq_z
    inverse = 1.0 / (sq + (zsq + 1.0))
    power = (cos_c * (sq - zsq) + sin_c * (along * freq_z)) * inverse + cos_w
    return 1.0 / (1.0 + jnp.exp2(power))


def by_lane(values, width):
    lane = iota((1, width), 1)
    row = jnp.zeros((1, width), f32)
    for i, value in enumerate(values):
        row = jnp.where(lane == i, f32(value), row)
    return row


def turns(orient, low_bin, high_bin, width):
    quarter = 0.5 * math.pi
    bin_ = 1.5 * math.pi / 180.0
    wide = 80.0 * math.pi / 180.0
    scale = GAIN * LOG2E
    turn = (
        orient * by_lane([2.0 * math.pi / ORIENTS] * 2, width)
        + low_bin * by_lane([0.0, 0.0, -bin_, -bin_, bin_], width)
        + high_bin * by_lane([0.0, 0.0, bin_, bin_, bin_], width)
        + by_lane([0.0, quarter, quarter, 0.0, quarter + wide], width)
    )
    return jnp.sin(turn) * by_lane([1.0, 1.0, -scale, 2.0 * scale, scale], width)


def to_column(row):
    size = row.shape[1]
    same = iota((size, size), 0) == iota((size, size), 1)
    return jnp.sum(jnp.where(same, row, 0.0), axis=1, keepdims=True)


def pack_kernel(
    padded, ref_hbm, cls_hbm, orient_hbm, tilt_hbm, packet_ref,
    ref_buf, cls_ref, orient_ref, tilt_ref, pack, in_sems, sems,
):
    coef = ref_hbm.shape[2]
    parts = orient_ref.shape[0]
    loads = [
        pltpu.make_async_copy(source, target, in_sems.at[i])
        for i, (source, target) in enumerate(
            ((ref_hbm, ref_buf), (cls_hbm, cls_ref), (orient_hbm, orient_ref), (tilt_hbm, tilt_ref))
        )
    ]
    for copy in loads:
        copy.start()
    for copy in loads:
        copy.wait()
    cls = cls_ref[...].reshape(1, parts)
    orient = orient_ref[...].reshape(1, parts)
    first = jnp.where(iota((2, parts), 0) == 0, cls, orient).astype(f32).astype(bf16)
    second = tilt_ref[...].astype(f32).astype(bf16)
    source, lane = iota((parts, LANES), 0), iota((parts, LANES), 1)
    labels = dot(first, (lane == source).astype(bf16)) + dot(
        second, (lane == source + parts).astype(bf16)
    )
    pack[:, padded - LANES : padded] = jnp.zeros((2, LANES), bf16)
    pack[:, 0:coef] = ref_buf[0]
    pack[:, padded : padded + LANES] = labels.astype(bf16)
    copies = [
        pltpu.make_async_copy(pack, packet_ref.at[q], sems.at[q])
        for q in range(packet_ref.shape[0])
    ]
    for copy in copies:
        copy.start()
    for copy in copies:
        copy.wait()


def weights(coef, padded, x_ref, orient_ref, tilt_ref):
    parts = orient_ref.shape[0]
    orient = orient_ref[...].reshape(1, parts)
    turn = turns(
        to_column(orient.astype(f32)),
        to_column(tilt_ref[0:1, :].astype(f32)),
        to_column(tilt_ref[1:2, :].astype(f32)),
        LANES,
    )
    factors = [turn[:, i : i + 1] for i in range(5)]
    out_row, in_row = iota((2 * parts, 2 * parts), 0), iota((2 * parts, 2 * parts), 1)
    wanted = jnp.where(out_row < parts, 2 * out_row, 2 * (out_row - parts) + 1)
    split = (in_row == wanted).astype(bf16)
    for start in range(0, padded, STEP):
        width = min(STEP, padded - start)
        valid = min(STEP, coef - start)
        both = dot(split, x_ref[:, :, start : start + valid].reshape(2 * parts, valid))
        if valid < width:
            both = jnp.concatenate([both, jnp.zeros((2 * parts, width - valid), f32)], axis=1)
        index = (iota((1, width), 1) + start).astype(f32)
        wedge = wedge_of(*freqs(index), *factors)
        if valid < width:
            wedge = jnp.where(index < coef, wedge, 0.0)
        yield start, width, wedge, both[:parts], both[parts:]


def sums_kernel(
    coef, chips, rows, half, x_ref, cls_ref, orient_ref, tilt_ref, keep_ref, send_ref
):
    parts = orient_ref.shape[0]
    cls = cls_ref[...].reshape(1, parts)
    core = lax.axis_index("dom") % 2
    order = iota((2 * chips, parts), 0)
    order = jnp.where(order < chips, 2 * order + core, 2 * (order - chips) + 1 - core)
    hot = (order == cls).astype(bf16)
    padded = -(-coef // LANES) * LANES
    for start, width, wedge, real, imag in weights(coef, padded, x_ref, orient_ref, tilt_ref):
        tile = start // LANES
        for part, value in enumerate((real, imag)):
            summed = dot(hot, (wedge * value).astype(bf16))
            for j in range(width // LANES):
                for q in range(0, chips, 8):
                    place = pl.ds(q * rows + part * half + tile + j, 8, stride=rows)
                    lanes = slice(j * LANES, (j + 1) * LANES)
                    keep_ref[place, :] = summed[q : q + 8, lanes]
                    send_ref[place, :] = summed[chips + q : chips + q + 8, lanes]


def weigh_kernel(coef, x_ref, orient_ref, tilt_ref, weighted_ref, low_ref, power_ref):
    parts, padded = low_ref.shape
    total = jnp.zeros(power_ref.shape, f32)
    for start, width, wedge, real, imag in weights(coef, padded, x_ref, orient_ref, tilt_ref):
        cols = slice(start, start + width)
        low_ref[:, cols] = wedge.astype(bf16)
        energy = wedge * (real * real + imag * imag)
        for j in range(width // LANES):
            total = total + energy[:, j * LANES : (j + 1) * LANES]
        weighted_ref[:parts, cols] = (wedge * real).astype(bf16)
        weighted_ref[parts:, cols] = (wedge * imag).astype(bf16)
    power_ref[...] = total


def add_kernel(chips, rows, room, keep_ref, got_ref, out_ref):
    for q in range(chips):
        place = pl.ds(q * rows, room)
        out_ref[q] = (keep_ref[place, :] + got_ref[place, :]).astype(bf16)


def join_kernel(*refs):
    *pieces, out_ref, sems = refs
    copies = [
        pltpu.make_async_copy(piece, out_ref.at[pl.ds(i * FAR, FAR)], sems.at[i])
        for i, piece in enumerate(pieces)
    ]
    for copy in copies:
        copy.start()
    for copy in copies:
        copy.wait()


def table_kernel(table_ref):
    for t in range(table_ref.shape[2] // LANES):
        index = (iota((8, LANES), 1) + t * LANES).astype(f32)
        for i, row in enumerate(freqs(index)):
            table_ref[i, :, t * LANES : (t + 1) * LANES] = row


def post_kernel(
    coef, same_ref, other_ref, weighted_ref, low_ref, power_ref, table,
    score_ref, load_ref, bottom_ref,
    squares, listed,
):
    chips = same_ref.shape[0]
    parts, padded = low_ref.shape
    devices = 2 * chips
    per_far = chips // FAR
    classes = score_ref.shape[1]
    tiles = padded // LANES
    me = lax.axis_index("dom")
    core = me % 2

    def picker(parity):
        out_row, in_row = iota((2 * devices, 2 * chips), 0), iota((2 * devices, 2 * chips), 1)
        part = (out_row >= devices).astype(i32)
        device = out_row - part * devices
        chip = device // 2
        near = (chip % per_far) ^ (me // 2 % per_far)
        far = (chip // per_far) ^ (me // 2 // per_far)
        place = near * FAR + far
        return (in_row == 2 * place + part) & (device % 2 == parity)

    pick_a, pick_b = picker(core).astype(bf16), picker(1 - core).astype(bf16)

    def rows_of(start, width):
        cols = pl.ds(start, width)
        a = same_ref[:, :, cols].reshape(2 * chips, width)
        b = other_ref[:, :, cols].reshape(2 * chips, width)
        return dot(pick_a, a) + dot(pick_b, b)

    labels = rows_of(padded, LANES)
    cls, orient = labels[:devices, :parts], labels[devices:, :parts]
    low_bin, high_bin = labels[:devices, parts : 2 * parts], labels[devices:, parts : 2 * parts]
    class_col = iota((classes, parts), 0).astype(f32)
    tally = jnp.zeros((classes, parts), f32)
    for r in range(devices):
        tally = tally + jnp.where(cls[r : r + 1] == class_col, 1.0, 0.0)
    tally = jnp.sum(tally, axis=1, keepdims=True)
    diagonal = iota((classes, classes), 0) == iota((classes, classes), 1)
    counts = jnp.sum(jnp.where(diagonal, tally, 0.0), axis=0, keepdims=True)
    load_ref[...] = counts * (classes / (devices * parts))

    chosen = cls == me.astype(f32)
    mask = chosen.astype(bf16)
    before = (iota((parts, parts), 0) < iota((parts, parts), 1)).astype(bf16)
    above = (iota((devices, devices), 0) > iota((devices, devices), 1)).astype(bf16)
    in_row = dot(mask, jnp.ones((parts, parts), bf16))
    rank = dot(mask, before) + dot(above, in_row.astype(bf16))
    rank = jnp.where(chosen, rank, -1.0)
    count = jnp.sum(jnp.where(chosen, 1.0, 0.0)).astype(i32)

    squares[...] = jnp.zeros_like(squares)

    def group(g, total):
        base = (g * GROUP).astype(f32)
        slot = iota((GROUP, parts), 0).astype(f32) + base
        values = [jnp.zeros((GROUP, 1), f32)] * 3
        columns = jnp.zeros((GROUP, 8), f32)
        pick = iota((8, parts), 0)
        for r in range(devices):
            hit = (rank[r : r + 1] == slot).astype(bf16)
            row = jnp.where(pick == 0, orient[r : r + 1], jnp.where(pick == 1, low_bin[r : r + 1], high_bin[r : r + 1]))
            columns = columns + dot_nt(hit, row.astype(bf16))
        turn = turns(columns[:, 0:1], columns[:, 1:2], columns[:, 2:3], 8)
        empty = iota((GROUP, 8), 0) + g * GROUP >= count
        listed[...] = jnp.where(empty & (iota((GROUP, 8), 1) == 4), 100.0, turn)
        left = jnp.minimum(count - g * GROUP, GROUP)

        def eight(e, total):
            params = listed[pl.ds(pl.multiple_of(e * 8, 8), 8), :]
            factors = [jnp.broadcast_to(params[:, i : i + 1], (8, LANES)) for i in range(5)]
            for t in range(tiles):
                cols = slice(t * LANES, (t + 1) * LANES)
                wedge = wedge_of(table[0, :, cols], table[1, :, cols], table[2, :, cols], *factors)
                squares[:, cols] += (wedge * wedge).astype(bf16).astype(f32)
                if (t + 1) * LANES > coef:
                    wedge = jnp.where(iota((8, LANES), 1) < coef - t * LANES, wedge, 0.0)
                total = total + wedge
            return total

        return lax.fori_loop(0, (left + 7) // 8, eight, total)

    total = lax.fori_loop(0, (count + GROUP - 1) // GROUP, group, jnp.zeros((8, LANES), f32))
    extra = TAU * (jnp.sum(total, keepdims=True) * (1.0 / coef) + 1.0)
    for t in range(tiles):
        cols = slice(t * LANES, (t + 1) * LANES)
        bottom_ref[t : t + 1, :] = jnp.sum(squares[:, cols], axis=0, keepdims=True) + extra

    intersection = jnp.zeros((parts, classes), f32)
    energy = jnp.zeros((parts, classes), f32)
    for start in range(0, padded, CHUNK):
        width = min(CHUNK, padded - start)
        cols = slice(start, start + width)
        both = rows_of(start, width)
        real, imag = both[:devices], both[devices:]
        ref_power = (real * real + imag * imag).astype(bf16)
        intersection = intersection + dot_nt(weighted_ref[:parts, cols], real.astype(bf16))
        intersection = intersection + dot_nt(weighted_ref[parts:, cols], imag.astype(bf16))
        energy = energy + dot_nt(low_ref[:, cols], ref_power)
    power = jnp.sum(power_ref[...], axis=1, keepdims=True)
    score_ref[...] = intersection / (
        math.sqrt(coef) * jnp.sqrt((energy / coef + EPS) * (power / coef + EPS))
    )


def final_kernel(coef, half, arrived_ref, bottom_ref, out_ref, ratio):
    tiles = -(-coef // LANES)
    total = arrived_ref[0].astype(f32)
    for q in range(1, arrived_ref.shape[0]):
        total = total + arrived_ref[q].astype(f32)
    bottom = bottom_ref[...]
    ratio[0:half, :] = total[0:half] / bottom[0:half]
    ratio[half : 2 * half, :] = total[half : 2 * half] / bottom[0:half]
    for t in range(tiles):
        width = min(LANES, coef - t * LANES)
        pair = ratio[pl.ds(t, 2, stride=half), :]
        out_ref[0, :, pl.ds(t * LANES, width)] = pair[:, :width]


def limit(*arrays):
    size = sum(math.prod(a.shape) * max(2, jnp.dtype(a.dtype).itemsize) for a in arrays)
    return pltpu.CompilerParams(vmem_limit_bytes=(4 << 20) + size)


def body(particles, references, assignment, orientation, tilt_range):
    part_rows = particles.shape[0]
    coef = particles.shape[2]
    owned = references.shape[0]
    devices = lax.axis_size("dom")
    chips = devices // 2
    classes = owned * devices
    assert owned == 1 and classes <= 256 and chips % 8 == 0 and chips & (chips - 1) == 0 and 2 * part_rows <= LANES
    groups = [[2 * q + c for q in range(chips)] for c in range(2)]
    near = devices // FAR
    swap = [(d, d ^ 1) for d in range(devices)]
    tiles = -(-coef // LANES)
    half = -(-tiles // 4) * 4
    room = 2 * half
    rows = room + 1
    padded = tiles * LANES
    wide = padded + LANES
    shape = jax.ShapeDtypeStruct
    hbm = pl.BlockSpec(memory_space=pltpu.HBM)
    vmem = pl.BlockSpec(memory_space=VMEM)

    cls = assignment.reshape(part_rows)
    packet = pl.pallas_call(
        functools.partial(pack_kernel, padded),
        out_shape=shape((1, 2, wide), bf16),
        in_specs=[hbm] * 4,
        out_specs=hbm,
        scratch_shapes=[
            VMEM(references.shape, bf16),
            VMEM((part_rows,), i32),
            VMEM((part_rows,), i32),
            VMEM(tilt_range.shape, i32),
            VMEM((2, wide), bf16),
            pltpu.SemaphoreType.DMA((4,)),
            pltpu.SemaphoreType.DMA((1,)),
        ],
        cost_estimate=pl.CostEstimate(flops=0, bytes_accessed=20 * 10**6, transcendentals=0),
        name="pack",
    )(references, cls, orientation, tilt_range)

    outs = (shape((chips * rows, LANES), f32), shape((chips * rows, LANES), f32))
    keep, send = pl.pallas_call(
        functools.partial(sums_kernel, coef, chips, rows, half),
        out_shape=outs,
        in_specs=[vmem] * 4,
        out_specs=(vmem, vmem),
        compiler_params=limit(*outs, particles),
        name="sums",
    )(particles, cls, orientation, tilt_range)
    got = lax.ppermute(send, "dom", swap)
    chip_sum = pl.pallas_call(
        functools.partial(add_kernel, chips, rows, room),
        out_shape=shape((chips, room, LANES), bf16),
        in_specs=[vmem, vmem],
        out_specs=vmem,
        compiler_params=limit(keep, got, keep),
        name="add",
    )(keep, got)
    arrived = lax.all_to_all(chip_sum, "dom", 0, 0, axis_index_groups=groups, tiled=True)
    pieces = [packet]
    for j in range(1, FAR):
        hop = [(d, d ^ (near * j)) for d in range(devices)]
        pieces.append(lax.ppermute(packet, "dom", hop))
    same = jnp.concatenate(pieces)
    outs = (
        shape((2 * part_rows, padded), bf16),
        shape((part_rows, padded), bf16),
        shape((part_rows, LANES), f32),
    )
    weighted, low, power = pl.pallas_call(
        functools.partial(weigh_kernel, coef),
        out_shape=outs,
        in_specs=[vmem] * 3,
        out_specs=(vmem, vmem, vmem),
        compiler_params=limit(*outs, particles),
        cost_estimate=pl.CostEstimate(flops=10**7, bytes_accessed=10**6, transcendentals=0),
        name="weigh",
    )(particles, orientation, tilt_range)
    table = pl.pallas_call(
        table_kernel,
        out_shape=shape((3, 8, padded), f32),
        out_specs=vmem,
        compiler_params=pltpu.CompilerParams(vmem_limit_bytes=4 << 20),
        name="table",
    )()
    pieces = [same]
    for j in range(1, chips // FAR):
        hop = [(d, d ^ (2 * j)) for d in range(devices)]
        pieces.append(lax.ppermute(same, "dom", hop))
    same = pl.pallas_call(
        join_kernel,
        out_shape=shape((chips, 2, wide), bf16),
        in_specs=[hbm] * len(pieces),
        out_specs=hbm,
        scratch_shapes=[pltpu.SemaphoreType.DMA((len(pieces),))],
        compiler_params=pltpu.CompilerParams(vmem_limit_bytes=4 << 20),
        name="join",
    )(*pieces)
    other = lax.ppermute(same, "dom", swap)

    outs = (
        shape((part_rows, classes), f32),
        shape((1, classes), f32),
        shape((-(-tiles // 8) * 8, LANES), f32),
    )
    scores, load, bottom = pl.pallas_call(
        functools.partial(post_kernel, coef),
        out_shape=outs,
        in_specs=[vmem] * 6,
        out_specs=(vmem, vmem, vmem),
        scratch_shapes=[
            VMEM((8, padded), f32),
            VMEM((GROUP, 8), f32),
        ],
        compiler_params=limit(same, other, weighted, low, table, *outs),
        name="post",
    )(same, other, weighted, low, power, table)

    class_means = pl.pallas_call(
        functools.partial(final_kernel, coef, half),
        out_shape=shape((owned, 2, coef), f32),
        in_specs=[vmem, vmem],
        out_specs=vmem,
        scratch_shapes=[VMEM((room, LANES), f32)],
        compiler_params=limit(arrived),
        name="means",
    )(arrived, bottom)
    return (scores, class_means, load.reshape(classes))


def solution(mesh):
    in_specs = (
        P("dom", None, None),
        P("dom", None, None),
        P("dom", None),
        P("dom"),
        P(None, "dom"),
    )
    out_specs = (P("dom", None), P("dom", None, None), P())
    return jax.shard_map(body, mesh=mesh, in_specs=in_specs, out_specs=out_specs, check_vma=False)
```

```python
import functools
import math

import jax
import jax.numpy as jnp
from jax import lax
from jax.experimental import pallas as pl
from jax.experimental.pallas import tpu as pltpu
from jax.sharding import PartitionSpec as P


GRID = 24
ORIENTS = 36

EPS = 1e-06
GAIN = 6.0
TAU = 0.5
LOG2E = math.log2(math.e)
LANES = 128
STEP = 512
CHUNK = 512
GROUP = 128
FAR = 4
VMEM = pltpu.VMEM
f32 = jnp.float32
bf16 = jnp.bfloat16
i32 = jnp.int32


def iota(shape, axis):
    return lax.broadcasted_iota(i32, shape, axis)


def dot(a, b):
    return jnp.dot(a, b, preferred_element_type=f32)


def dot_nt(a, b):
    return lax.dot_general(a, b, (((1,), (1,)), ((), ())), preferred_element_type=f32)


def freqs(index):
    plane = jnp.floor((index + 0.5) * (1.0 / (GRID * GRID)))
    rest = index - plane * (GRID * GRID)
    col_x = jnp.floor((rest + 0.5) * (1.0 / GRID))
    col_z = rest - col_x * GRID
    half = GRID // 2
    freq_x = jnp.where(col_x < half, col_x, col_x - GRID)
    freq_z = jnp.where(col_z < half, col_z, col_z - GRID)
    return freq_x, plane, freq_z


def wedge_of(freq_x, freq_y, freq_z, sin_a, cos_a, cos_c, sin_c, cos_w):
    along = freq_y * cos_a - freq_x * sin_a
    sq = along * along
    zsq = freq_z * freq_z
    inverse = 1.0 / (sq + (zsq + 1.0))
    power = (cos_c * (sq - zsq) + sin_c * (along * freq_z)) * inverse + cos_w
    return 1.0 / (1.0 + jnp.exp2(power))


def by_lane(values, width):
    lane = iota((1, width), 1)
    row = jnp.zeros((1, width), f32)
    for i, value in enumerate(values):
        row = jnp.where(lane == i, f32(value), row)
    return row


def turns(orient, low_bin, high_bin, width):
    quarter = 0.5 * math.pi
    bin_ = 1.5 * math.pi / 180.0
    wide = 80.0 * math.pi / 180.0
    scale = GAIN * LOG2E
    turn = (
        orient * by_lane([2.0 * math.pi / ORIENTS] * 2, width)
        + low_bin * by_lane([0.0, 0.0, -bin_, -bin_, bin_], width)
        + high_bin * by_lane([0.0, 0.0, bin_, bin_, bin_], width)
        + by_lane([0.0, quarter, quarter, 0.0, quarter + wide], width)
    )
    return jnp.sin(turn) * by_lane([1.0, 1.0, -scale, 2.0 * scale, scale], width)


def to_column(row):
    size = row.shape[1]
    same = iota((size, size), 0) == iota((size, size), 1)
    return jnp.sum(jnp.where(same, row, 0.0), axis=1, keepdims=True)


def weights(coef, padded, x_ref, label_ref):
    parts = label_ref.shape[1]
    turn = turns(*[to_column(label_ref[i : i + 1, :].astype(f32)) for i in (1, 2, 3)], LANES)
    factors = [turn[:, i : i + 1] for i in range(5)]
    out_row, in_row = iota((2 * parts, 2 * parts), 0), iota((2 * parts, 2 * parts), 1)
    wanted = jnp.where(out_row < parts, 2 * out_row, 2 * (out_row - parts) + 1)
    split = (in_row == wanted).astype(bf16)
    for start in range(0, padded, STEP):
        width = min(STEP, padded - start)
        valid = min(STEP, coef - start)
        both = dot(split, x_ref[:, :, start : start + valid].reshape(2 * parts, valid))
        if valid < width:
            both = jnp.concatenate([both, jnp.zeros((2 * parts, width - valid), f32)], axis=1)
        index = (iota((1, width), 1) + start).astype(f32)
        wedge = wedge_of(*freqs(index), *factors)
        if valid < width:
            wedge = jnp.where(index < coef, wedge, 0.0)
        yield start, width, wedge, both[:parts], both[parts:]


def sums_kernel(
    coef, chips, rows, half, x_ref, ref_ref, label_ref, packet_ref, keep_ref, send_ref
):
    parts = label_ref.shape[1]
    padded = -(-coef // LANES) * LANES
    cls = label_ref[0:1, :]

    first = label_ref[0:2, :].astype(f32).astype(bf16)
    second = label_ref[2:4, :].astype(f32).astype(bf16)
    source, lane = iota((parts, LANES), 0), iota((parts, LANES), 1)
    labels = dot(first, (lane == source).astype(bf16)) + dot(
        second, (lane == source + parts).astype(bf16)
    )
    packet_ref[0, :, padded - LANES : padded] = jnp.zeros((2, LANES), bf16)
    packet_ref[0, :, 0:coef] = ref_ref[0]
    packet_ref[0, :, padded : padded + LANES] = labels.astype(bf16)

    me = lax.axis_index("dom")
    core, chip = me % 2, me // 2
    nears = chips // FAR
    row = iota((2 * chips, parts), 0)
    place = row % chips
    q = ((place % FAR) ^ (chip // nears)) * nears + ((place // FAR) ^ (chip % nears))
    order = 2 * q + jnp.where(row < chips, core, 1 - core)
    hot = (order == cls).astype(bf16)
    for start, width, wedge, real, imag in weights(coef, padded, x_ref, label_ref):
        tile = start // LANES
        for part, value in enumerate((real, imag)):
            summed = dot(hot, (wedge * value).astype(bf16))
            for j in range(width // LANES):
                for q in range(0, chips, 8):
                    place = pl.ds(q * rows + part * half + tile + j, 8, stride=rows)
                    lanes = slice(j * LANES, (j + 1) * LANES)
                    keep_ref[place, :] = summed[q : q + 8, lanes]
                    send_ref[place, :] = summed[chips + q : chips + q + 8, lanes]


def weigh_kernel(coef, x_ref, label_ref, weighted_ref, low_ref, power_ref):
    parts, padded = low_ref.shape
    total = jnp.zeros(power_ref.shape, f32)
    for start, width, wedge, real, imag in weights(coef, padded, x_ref, label_ref):
        cols = slice(start, start + width)
        low_ref[:, cols] = wedge.astype(bf16)
        energy = wedge * (real * real + imag * imag)
        for j in range(width // LANES):
            total = total + energy[:, j * LANES : (j + 1) * LANES]
        weighted_ref[:parts, cols] = (wedge * real).astype(bf16)
        weighted_ref[parts:, cols] = (wedge * imag).astype(bf16)
    power_ref[...] = total


def core_kernel(rows, keep_ref, got_ref, *outs):
    room = outs[0].shape[1]
    for r in range(len(outs) * FAR):
        place = pl.ds(r * rows, room)
        out_ref = outs[r // FAR]
        out_ref[r % FAR] = (keep_ref[place, :] + got_ref[place, :]).astype(out_ref.dtype)


def near_kernel(*refs):
    own_ref, *came = refs[:-FAR]
    outs = refs[-FAR:]
    for k, out_ref in enumerate(outs):
        total = own_ref[k]
        for came_ref in came:
            total = total + came_ref[k].astype(f32)
        out_ref[0] = total.astype(out_ref.dtype)


def join(pieces):
    size, *rest = pieces[0].shape
    hbm = pl.BlockSpec(memory_space=pltpu.HBM)
    return pl.pallas_call(
        join_kernel,
        out_shape=jax.ShapeDtypeStruct((size * len(pieces), *rest), pieces[0].dtype),
        in_specs=[hbm] * len(pieces),
        out_specs=hbm,
        scratch_shapes=[pltpu.SemaphoreType.DMA((len(pieces),))],
        compiler_params=pltpu.CompilerParams(vmem_limit_bytes=4 << 20),
        name="join",
    )(*pieces)


def join_kernel(*refs):
    *pieces, out_ref, sems = refs
    size = pieces[0].shape[0]
    copies = [
        pltpu.make_async_copy(piece, out_ref.at[pl.ds(i * size, size)], sems.at[i])
        for i, piece in enumerate(pieces)
    ]
    for copy in copies:
        copy.start()
    for copy in copies:
        copy.wait()


def table_kernel(table_ref):
    for t in range(table_ref.shape[2] // LANES):
        index = (iota((8, LANES), 1) + t * LANES).astype(f32)
        for i, row in enumerate(freqs(index)):
            table_ref[i, :, t * LANES : (t + 1) * LANES] = row


def post_kernel(
    coef, same_ref, other_ref, weighted_ref, low_ref, power_ref, table,
    score_ref, load_ref, bottom_ref,
    squares, listed,
):
    chips = same_ref.shape[0]
    parts, padded = low_ref.shape
    devices = 2 * chips
    per_far = chips // FAR
    classes = score_ref.shape[1]
    tiles = padded // LANES
    me = lax.axis_index("dom")
    core = me % 2

    def picker(parity):
        out_row, in_row = iota((2 * devices, 2 * chips), 0), iota((2 * devices, 2 * chips), 1)
        part = (out_row >= devices).astype(i32)
        device = out_row - part * devices
        chip = device // 2
        near = (chip % per_far) ^ (me // 2 % per_far)
        far = (chip // per_far) ^ (me // 2 // per_far)
        place = near * FAR + far
        return (in_row == 2 * place + part) & (device % 2 == parity)

    pick_a, pick_b = picker(core).astype(bf16), picker(1 - core).astype(bf16)

    def rows_of(start, width):
        cols = pl.ds(start, width)
        a = same_ref[:, :, cols].reshape(2 * chips, width)
        b = other_ref[:, :, cols].reshape(2 * chips, width)
        return dot(pick_a, a) + dot(pick_b, b)

    labels = rows_of(padded, LANES)
    cls, orient = labels[:devices, :parts], labels[devices:, :parts]
    low_bin, high_bin = labels[:devices, parts : 2 * parts], labels[devices:, parts : 2 * parts]
    class_col = iota((classes, parts), 0).astype(f32)
    tally = jnp.zeros((classes, parts), f32)
    for r in range(devices):
        tally = tally + jnp.where(cls[r : r + 1] == class_col, 1.0, 0.0)
    tally = jnp.sum(tally, axis=1, keepdims=True)
    diagonal = iota((classes, classes), 0) == iota((classes, classes), 1)
    counts = jnp.sum(jnp.where(diagonal, tally, 0.0), axis=0, keepdims=True)
    load_ref[...] = counts * (classes / (devices * parts))

    chosen = cls == me.astype(f32)
    mask = chosen.astype(bf16)
    before = (iota((parts, parts), 0) < iota((parts, parts), 1)).astype(bf16)
    above = (iota((devices, devices), 0) > iota((devices, devices), 1)).astype(bf16)
    in_row = dot(mask, jnp.ones((parts, parts), bf16))
    rank = dot(mask, before) + dot(above, in_row.astype(bf16))
    rank = jnp.where(chosen, rank, -1.0)
    count = jnp.sum(jnp.where(chosen, 1.0, 0.0)).astype(i32)

    squares[...] = jnp.zeros_like(squares)

    def group(g, total):
        base = (g * GROUP).astype(f32)
        slot = iota((GROUP, parts), 0).astype(f32) + base
        values = [jnp.zeros((GROUP, 1), f32)] * 3
        columns = jnp.zeros((GROUP, 8), f32)
        pick = iota((8, parts), 0)
        for r in range(devices):
            hit = (rank[r : r + 1] == slot).astype(bf16)
            row = jnp.where(pick == 0, orient[r : r + 1], jnp.where(pick == 1, low_bin[r : r + 1], high_bin[r : r + 1]))
            columns = columns + dot_nt(hit, row.astype(bf16))
        turn = turns(columns[:, 0:1], columns[:, 1:2], columns[:, 2:3], 8)
        empty = iota((GROUP, 8), 0) + g * GROUP >= count
        listed[...] = jnp.where(empty & (iota((GROUP, 8), 1) == 4), 100.0, turn)
        left = jnp.minimum(count - g * GROUP, GROUP)

        def eight(e, total):
            params = listed[pl.ds(pl.multiple_of(e * 8, 8), 8), :]
            factors = [jnp.broadcast_to(params[:, i : i + 1], (8, LANES)) for i in range(5)]
            for t in range(tiles):
                cols = slice(t * LANES, (t + 1) * LANES)
                wedge = wedge_of(table[0, :, cols], table[1, :, cols], table[2, :, cols], *factors)
                squares[:, cols] += (wedge * wedge).astype(bf16).astype(f32)
                if (t + 1) * LANES > coef:
                    wedge = jnp.where(iota((8, LANES), 1) < coef - t * LANES, wedge, 0.0)
                total = total + wedge
            return total

        return lax.fori_loop(0, (left + 7) // 8, eight, total)

    total = lax.fori_loop(0, (count + GROUP - 1) // GROUP, group, jnp.zeros((8, LANES), f32))
    extra = TAU * (jnp.sum(total, keepdims=True) * (1.0 / coef) + 1.0)
    for t in range(tiles):
        cols = slice(t * LANES, (t + 1) * LANES)
        bottom_ref[t : t + 1, :] = jnp.sum(squares[:, cols], axis=0, keepdims=True) + extra

    intersection = jnp.zeros((parts, classes), f32)
    energy = jnp.zeros((parts, classes), f32)
    for start in range(0, padded, CHUNK):
        width = min(CHUNK, padded - start)
        cols = slice(start, start + width)
        both = rows_of(start, width)
        real, imag = both[:devices], both[devices:]
        ref_power = (real * real + imag * imag).astype(bf16)
        intersection = intersection + dot_nt(weighted_ref[:parts, cols], real.astype(bf16))
        intersection = intersection + dot_nt(weighted_ref[parts:, cols], imag.astype(bf16))
        energy = energy + dot_nt(low_ref[:, cols], ref_power)
    power = jnp.sum(power_ref[...], axis=1, keepdims=True)
    score_ref[...] = intersection / (
        math.sqrt(coef) * jnp.sqrt((energy / coef + EPS) * (power / coef + EPS))
    )


def final_kernel(coef, half, *refs):
    own_ref, *came, bottom_ref, out_ref, ratio = refs
    tiles = -(-coef // LANES)
    total = own_ref[0]
    for came_ref in came:
        total = total + came_ref[0].astype(f32)
    bottom = bottom_ref[...]
    ratio[0:half, :] = total[0:half] / bottom[0:half]
    ratio[half : 2 * half, :] = total[half : 2 * half] / bottom[0:half]
    for t in range(tiles):
        width = min(LANES, coef - t * LANES)
        pair = ratio[pl.ds(t, 2, stride=half), :]
        out_ref[0, :, pl.ds(t * LANES, width)] = pair[:, :width]


def limit(*arrays):
    size = sum(math.prod(a.shape) * max(2, jnp.dtype(a.dtype).itemsize) for a in arrays)
    return pltpu.CompilerParams(vmem_limit_bytes=(4 << 20) + size)


def body(particles, references, assignment, orientation, tilt_range):
    part_rows = particles.shape[0]
    coef = particles.shape[2]
    owned = references.shape[0]
    devices = lax.axis_size("dom")
    chips = devices // 2
    classes = owned * devices
    assert owned == 1 and classes <= 256 and chips % 8 == 0 and chips & (chips - 1) == 0 and 2 * part_rows <= LANES
    tiles = -(-coef // LANES)
    half = -(-tiles // 4) * 4
    room = 2 * half
    rows = room + 1
    padded = tiles * LANES
    wide = padded + LANES
    shape = jax.ShapeDtypeStruct
    vmem = pl.BlockSpec(memory_space=VMEM)

    labels = jnp.concatenate([assignment.reshape(1, -1), orientation.reshape(1, -1), tilt_range])
    nears = chips // FAR

    def hops(step):
        return [(d, d ^ step) for d in range(devices)]

    outs = (
        shape((1, 2, wide), bf16),
        shape((chips * rows, LANES), f32),
        shape((chips * rows, LANES), f32),
    )
    packet, keep, send = pl.pallas_call(
        functools.partial(sums_kernel, coef, chips, rows, half),
        out_shape=outs,
        in_specs=[vmem] * 3,
        out_specs=(vmem,) * 3,
        compiler_params=limit(*outs, particles),
        name="sums",
    )(particles, references, labels)
    got = lax.ppermute(send, "dom", hops(1))
    pieces = [packet]
    for k in range(1, FAR):
        pieces.append(lax.ppermute(packet, "dom", hops(2 * nears * k)))
    outs = [shape((FAR, room, LANES), f32 if j == 0 else bf16) for j in range(nears)]
    own, *leave = pl.pallas_call(
        functools.partial(core_kernel, rows),
        out_shape=outs,
        in_specs=[vmem] * 2,
        out_specs=[vmem] * nears,
        compiler_params=limit(keep, got, *outs),
        name="core_add",
    )(keep, got)
    came = []
    for j in range(1, nears):
        came.append(lax.ppermute(leave[j - 1], "dom", hops(2 * j)))
    outs = [shape((1, room, LANES), f32 if k == 0 else bf16) for k in range(FAR)]
    own, *leave = pl.pallas_call(
        near_kernel,
        out_shape=outs,
        in_specs=[vmem] * nears,
        out_specs=[vmem] * FAR,
        compiler_params=limit(own, *came, *outs),
        name="near_add",
    )(own, *came)
    came = []
    for k in range(1, FAR):
        came.append(lax.ppermute(leave[k - 1], "dom", hops(2 * nears * k)))
    same = join(pieces)
    outs = (
        shape((2 * part_rows, padded), bf16),
        shape((part_rows, padded), bf16),
        shape((part_rows, LANES), f32),
    )
    weighted, low, power = pl.pallas_call(
        functools.partial(weigh_kernel, coef),
        out_shape=outs,
        in_specs=[vmem] * 2,
        out_specs=(vmem, vmem, vmem),
        compiler_params=limit(*outs, particles),
        cost_estimate=pl.CostEstimate(flops=10**7, bytes_accessed=10**6, transcendentals=0),
        name="weigh",
    )(particles, labels)
    table = pl.pallas_call(
        table_kernel,
        out_shape=shape((3, 8, padded), f32),
        out_specs=vmem,
        compiler_params=pltpu.CompilerParams(vmem_limit_bytes=4 << 20),
        name="table",
    )()
    pieces = [same]
    for j in range(1, nears):
        pieces.append(lax.ppermute(same, "dom", hops(2 * j)))
    same = join(pieces)
    other = lax.ppermute(same, "dom", hops(1))

    outs = (
        shape((part_rows, classes), f32),
        shape((1, classes), f32),
        shape((-(-tiles // 8) * 8, LANES), f32),
    )
    scores, load, bottom = pl.pallas_call(
        functools.partial(post_kernel, coef),
        out_shape=outs,
        in_specs=[vmem] * 6,
        out_specs=(vmem, vmem, vmem),
        scratch_shapes=[
            VMEM((8, padded), f32),
            VMEM((GROUP, 8), f32),
        ],
        compiler_params=limit(same, other, weighted, low, table, *outs),
        name="post",
    )(same, other, weighted, low, power, table)

    class_means = pl.pallas_call(
        functools.partial(final_kernel, coef, half),
        out_shape=shape((owned, 2, coef), f32),
        in_specs=[vmem] * (FAR + 1),
        out_specs=vmem,
        scratch_shapes=[VMEM((room, LANES), f32)],
        compiler_params=pltpu.CompilerParams(vmem_limit_bytes=4 << 20),
        name="means",
    )(own, *came, bottom)
    return (scores, class_means, load.reshape(classes))


def solution(mesh):
    in_specs = (
        P("dom", None, None),
        P("dom", None, None),
        P("dom", None),
        P("dom"),
        P(None, "dom"),
    )
    out_specs = (P("dom", None), P("dom", None, None), P())
    return jax.shard_map(body, mesh=mesh, in_specs=in_specs, out_specs=out_specs, check_vma=False)
```

```python
import functools
import math

import jax
import jax.numpy as jnp
from jax import lax
from jax.experimental import pallas as pl
from jax.experimental.pallas import tpu as pltpu
from jax.sharding import PartitionSpec as P


GRID = 24
ORIENTS = 36

EPS = 1e-06
GAIN = 6.0
TAU = 0.5
LOG2E = math.log2(math.e)
LANES = 128
STEP = 512
CHUNK = 512
GROUP = 128
FAR = 4
PIECES = 1
VMEM = pltpu.VMEM
f32 = jnp.float32
bf16 = jnp.bfloat16
i32 = jnp.int32


def iota(shape, axis):
    return lax.broadcasted_iota(i32, shape, axis)


def dot(a, b):
    return jnp.dot(a, b, preferred_element_type=f32)


def dot_nt(a, b):
    return lax.dot_general(a, b, (((1,), (1,)), ((), ())), preferred_element_type=f32)


def freqs(index):
    plane = jnp.floor((index + 0.5) * (1.0 / (GRID * GRID)))
    rest = index - plane * (GRID * GRID)
    col_x = jnp.floor((rest + 0.5) * (1.0 / GRID))
    col_z = rest - col_x * GRID
    half = GRID // 2
    freq_x = jnp.where(col_x < half, col_x, col_x - GRID)
    freq_z = jnp.where(col_z < half, col_z, col_z - GRID)
    return freq_x, plane, freq_z


def wedge_of(freq_x, freq_y, freq_z, sin_a, cos_a, cos_c, sin_c, cos_w):
    along = freq_y * cos_a - freq_x * sin_a
    sq = along * along
    zsq = freq_z * freq_z
    inverse = 1.0 / (sq + (zsq + 1.0))
    power = (cos_c * (sq - zsq) + sin_c * (along * freq_z)) * inverse + cos_w
    return 1.0 / (1.0 + jnp.exp2(power))


def by_lane(values, width):
    lane = iota((1, width), 1)
    row = jnp.zeros((1, width), f32)
    for i, value in enumerate(values):
        row = jnp.where(lane == i, f32(value), row)
    return row


def turns(orient, low_bin, high_bin, width):
    quarter = 0.5 * math.pi
    bin_ = 1.5 * math.pi / 180.0
    wide = 80.0 * math.pi / 180.0
    scale = GAIN * LOG2E
    turn = (
        orient * by_lane([2.0 * math.pi / ORIENTS] * 2, width)
        + low_bin * by_lane([0.0, 0.0, -bin_, -bin_, bin_], width)
        + high_bin * by_lane([0.0, 0.0, bin_, bin_, bin_], width)
        + by_lane([0.0, quarter, quarter, 0.0, quarter + wide], width)
    )
    return jnp.sin(turn) * by_lane([1.0, 1.0, -scale, 2.0 * scale, scale], width)


def to_column(row):
    size = row.shape[1]
    same = iota((size, size), 0) == iota((size, size), 1)
    return jnp.sum(jnp.where(same, row, 0.0), axis=1, keepdims=True)


def weights(coef, padded, read, label_ref):
    parts = label_ref.shape[1]
    turn = turns(*[to_column(label_ref[i : i + 1, :].astype(f32)) for i in (1, 2, 3)], LANES)
    factors = [turn[:, i : i + 1] for i in range(5)]
    out_row, in_row = iota((2 * parts, 2 * parts), 0), iota((2 * parts, 2 * parts), 1)
    wanted = jnp.where(out_row < parts, 2 * out_row, 2 * (out_row - parts) + 1)
    split = (in_row == wanted).astype(bf16)
    for start in range(0, padded, STEP):
        width = min(STEP, padded - start)
        valid = min(STEP, coef - start)
        both = dot(split, read(start, valid))
        if valid < width:
            both = jnp.concatenate([both, jnp.zeros((2 * parts, width - valid), f32)], axis=1)
        index = (iota((1, width), 1) + start).astype(f32)
        wedge = wedge_of(*freqs(index), *factors)
        if valid < width:
            wedge = jnp.where(index < coef, wedge, 0.0)
        yield start, width, wedge, both[:parts], both[parts:]


def sums_kernel(
    coef, chips, rows, half, x_hbm, ref_hbm, cls_hbm, orient_hbm, tilt_hbm,
    packet_ref, keep_ref, send_ref, label_ref,
    x_ref, ref_ref, cls_ref, orient_ref, tilt_ref, in_sems, x_sems,
):
    parts = label_ref.shape[1]
    padded = -(-coef // LANES) * LANES
    pairs = ((cls_hbm, cls_ref), (orient_hbm, orient_ref), (tilt_hbm, tilt_ref), (ref_hbm, ref_ref))
    loads = [pltpu.make_async_copy(a, b, in_sems.at[i]) for i, (a, b) in enumerate(pairs)]
    for copy in loads:
        copy.start()
    pieces = x_sems.shape[0]
    span = -(-coef // (STEP * pieces)) * STEP
    copies = []
    for i in range(pieces):
        cols = pl.ds(i * span, min(span, coef - i * span))
        copies.append(
            pltpu.make_async_copy(x_hbm.at[:, :, cols], x_ref.at[:, :, cols], x_sems.at[i])
        )
        copies[-1].start()
    for copy in loads:
        copy.wait()
    label_ref[0:1, :] = cls_ref[...].reshape(1, parts)
    label_ref[1:2, :] = orient_ref[...].reshape(1, parts)
    label_ref[2:4, :] = tilt_ref[...]
    cls = label_ref[0:1, :]

    def read(start, valid):
        if start % span == 0:
            copies[start // span].wait()
        return x_ref[:, :, start : start + valid].reshape(2 * parts, valid)


    spread = (iota((parts, LANES), 1) % parts == iota((parts, LANES), 0)).astype(bf16)
    repeated = dot(label_ref[...].astype(f32).astype(bf16), spread)
    lane = iota(repeated.shape, 1) // parts
    row = jnp.sum(jnp.where(lane == iota(repeated.shape, 0), repeated, 0.0), axis=0, keepdims=True)
    labels = jnp.where(iota((2, LANES), 0) == 0, row, -1.0)
    packet_ref[0, :, padded - LANES : padded] = jnp.zeros((2, LANES), bf16)
    packet_ref[0, :, 0:coef] = ref_ref[0]
    packet_ref[0, :, padded : padded + LANES] = labels.astype(bf16)

    me = lax.axis_index("dom")
    core, chip = me % 2, me // 2
    nears = chips // FAR
    row = iota((2 * chips, parts), 0)
    place = row % chips
    q = ((place % FAR) ^ (chip // nears)) * nears + ((place // FAR) ^ (chip % nears))
    order = 2 * q + jnp.where(row < chips, core, 1 - core)
    hot = (order == cls).astype(bf16)
    for start, width, wedge, real, imag in weights(coef, padded, read, label_ref):
        tile = start // LANES
        for part, value in enumerate((real, imag)):
            summed = dot(hot, (wedge * value).astype(bf16))
            for j in range(width // LANES):
                for q in range(0, chips, 8):
                    place = pl.ds(q * rows + part * half + tile + j, 8, stride=rows)
                    lanes = slice(j * LANES, (j + 1) * LANES)
                    keep_ref[place, :] = summed[q : q + 8, lanes]
                    send_ref[place, :] = summed[chips + q : chips + q + 8, lanes]


def weigh_kernel(coef, x_ref, label_ref, weighted_ref, low_ref, power_ref):
    parts, padded = low_ref.shape
    total = jnp.zeros(power_ref.shape, f32)

    def read(start, valid):
        return x_ref[:, :, start : start + valid].reshape(2 * parts, valid)

    for start, width, wedge, real, imag in weights(coef, padded, read, label_ref):
        cols = slice(start, start + width)
        low_ref[:, cols] = wedge.astype(bf16)
        energy = wedge * (real * real + imag * imag)
        for j in range(width // LANES):
            total = total + energy[:, j * LANES : (j + 1) * LANES]
        weighted_ref[:parts, cols] = (wedge * real).astype(bf16)
        weighted_ref[parts:, cols] = (wedge * imag).astype(bf16)
    power_ref[...] = total


def core_kernel(rows, keep_ref, got_ref, *outs):
    room = outs[0].shape[1]
    for r in range(len(outs) * FAR):
        place = pl.ds(r * rows, room)
        out_ref = outs[r // FAR]
        out_ref[r % FAR] = (keep_ref[place, :] + got_ref[place, :]).astype(out_ref.dtype)


def near_kernel(*refs):
    own_ref, *came = refs[:-FAR]
    outs = refs[-FAR:]
    for k, out_ref in enumerate(outs):
        total = own_ref[k]
        for came_ref in came:
            total = total + came_ref[k].astype(f32)
        out_ref[0] = total.astype(out_ref.dtype)


def join(pieces):
    size, *rest = pieces[0].shape
    hbm = pl.BlockSpec(memory_space=pl.ANY)
    return pl.pallas_call(
        join_kernel,
        out_shape=jax.ShapeDtypeStruct((size * len(pieces), *rest), pieces[0].dtype),
        in_specs=[hbm] * len(pieces),
        out_specs=hbm,
        scratch_shapes=[pltpu.SemaphoreType.DMA((len(pieces),))],
        compiler_params=pltpu.CompilerParams(vmem_limit_bytes=4 << 20),
        name="join",
    )(*pieces)


def join_kernel(*refs):
    *pieces, out_ref, sems = refs
    size = pieces[0].shape[0]
    copies = [
        pltpu.make_async_copy(piece, out_ref.at[pl.ds(i * size, size)], sems.at[i])
        for i, piece in enumerate(pieces)
    ]
    for copy in copies:
        copy.start()
    for copy in copies:
        copy.wait()


def table_kernel(table_ref):
    for t in range(table_ref.shape[2] // LANES):
        index = (iota((8, LANES), 1) + t * LANES).astype(f32)
        for i, row in enumerate(freqs(index)):
            table_ref[i, :, t * LANES : (t + 1) * LANES] = row


def device_of(place, nears, flip):
    me = lax.axis_index("dom")
    chip = me // 2
    far, near = place % FAR, place // FAR
    return 2 * ((far ^ (chip // nears)) * nears + (near ^ (chip % nears))) + me % 2 * (
        1 - 2 * flip
    ) + flip


def match(block_ref, weighted_ref, low_ref, flip):
    chips = block_ref.shape[0]
    parts, padded = low_ref.shape
    devices = 2 * chips
    inter = jnp.zeros((2 * parts, devices), f32)
    energy = jnp.zeros((parts, devices), f32)
    for start in range(0, padded, CHUNK):
        width = min(CHUNK, padded - start)
        cols = slice(start, start + width)
        rows = block_ref[:, :, cols].reshape(devices, width)
        inter = inter + dot_nt(weighted_ref[:, cols], rows)
        square = rows.astype(f32) * rows.astype(f32)
        pair = square + pltpu.roll(square, devices - 1, 0)
        energy = energy + dot_nt(low_ref[:, cols], pair.astype(bf16))
    row, column = iota((devices, devices), 0), iota((devices, devices), 1)
    here = device_of(row // 2, chips // FAR, flip) == column
    real = (here & (row % 2 == 0)).astype(f32)
    imag = (here & (row % 2 == 1)).astype(f32)

    def pick(a, b):
        return jnp.dot(a, b, precision=lax.Precision.HIGHEST, preferred_element_type=f32)

    return pick(inter[:parts], real) + pick(inter[parts:], imag), pick(energy, real)


def own_kernel(same_ref, weighted_ref, low_ref, inter_ref, energy_ref):
    inter_ref[...], energy_ref[...] = match(same_ref, weighted_ref, low_ref, 0)


def post_kernel(
    coef, same_ref, other_ref, weighted_ref, low_ref, power_ref, table, inter_ref, energy_ref,
    score_ref, load_ref, bottom_ref,
    squares, listed,
):
    chips = same_ref.shape[0]
    parts, padded = low_ref.shape
    devices = 2 * chips
    classes = score_ref.shape[1]
    tiles = padded // LANES
    me = lax.axis_index("dom")

    cols = slice(padded, padded + LANES)
    labels = jnp.concatenate(
        [ref[:, :, cols].reshape(2 * chips, LANES).astype(f32) for ref in (same_ref, other_ref)]
    )
    every = labels.shape[0]
    cls = labels[:, :parts]

    class_col = iota((classes, parts), 0).astype(f32)
    tally = jnp.zeros((classes, parts), f32)
    for r in range(0, every, 2):
        tally = tally + jnp.where(cls[r : r + 1] == class_col, 1.0, 0.0)
    tally = jnp.sum(tally, axis=1, keepdims=True)
    diagonal = iota((classes, classes), 0) == iota((classes, classes), 1)
    counts = jnp.sum(jnp.where(diagonal, tally, 0.0), axis=0, keepdims=True)
    load_ref[...] = counts * (classes / (devices * parts))

    chosen = cls == me.astype(f32)
    mask = chosen.astype(bf16)
    before = (iota((parts, parts), 0) < iota((parts, parts), 1)).astype(bf16)
    rank = jnp.where(chosen, dot(mask, before), -1.0).astype(bf16)
    held = dot(mask, jnp.ones((parts, every), bf16))
    earlier, later = iota((every, every), 0), iota((every, every), 1)
    start = jnp.sum(jnp.where(earlier < later, held, 0.0), axis=0, keepdims=True)
    stop = jnp.sum(jnp.where(earlier <= later, held, 0.0), axis=0, keepdims=True)
    count = jnp.sum(jnp.where(chosen, 1.0, 0.0)).astype(i32)
    spread = (iota((parts, LANES), 1) % parts == iota((parts, LANES), 0)).astype(bf16)
    gather = (iota((LANES, 8), 0) // parts == iota((LANES, 8), 1) + 1).astype(bf16)

    squares[...] = jnp.zeros_like(squares)

    def group(g, total):
        slot = iota((GROUP, 1), 0).astype(f32) + (g * GROUP).astype(f32)
        in_row = (slot >= start) & (slot < stop)
        row = in_row.astype(bf16)
        within = slot - jnp.sum(jnp.where(in_row, start, 0.0), axis=1, keepdims=True)
        hit = dot((dot(row, rank) == within).astype(bf16), spread)
        columns = dot((hit * dot(row, labels.astype(bf16))).astype(bf16), gather)
        turn = turns(columns[:, 0:1], columns[:, 1:2], columns[:, 2:3], 8)
        empty = iota((GROUP, 8), 0) + g * GROUP >= count
        listed[...] = jnp.where(empty & (iota((GROUP, 8), 1) == 4), 100.0, turn)
        left = jnp.minimum(count - g * GROUP, GROUP)

        def eight(e, total):
            params = listed[pl.ds(pl.multiple_of(e * 8, 8), 8), :]
            factors = [jnp.broadcast_to(params[:, i : i + 1], (8, LANES)) for i in range(5)]
            for t in range(tiles):
                cols = slice(t * LANES, (t + 1) * LANES)
                wedge = wedge_of(table[0, :, cols], table[1, :, cols], table[2, :, cols], *factors)
                squares[:, cols] += (wedge * wedge).astype(bf16).astype(f32)
                if (t + 1) * LANES > coef:
                    wedge = jnp.where(iota((8, LANES), 1) < coef - t * LANES, wedge, 0.0)
                total = total + wedge
            return total

        return lax.fori_loop(0, (left + 7) // 8, eight, total)

    total = lax.fori_loop(0, (count + GROUP - 1) // GROUP, group, jnp.zeros((8, LANES), f32))
    extra = TAU * (jnp.sum(total, keepdims=True) * (1.0 / coef) + 1.0)
    for t in range(tiles):
        cols = slice(t * LANES, (t + 1) * LANES)
        bottom_ref[t : t + 1, :] = jnp.sum(squares[:, cols], axis=0, keepdims=True) + extra

    inter, energy = match(other_ref, weighted_ref, low_ref, 1)
    intersection = inter + inter_ref[...]
    energy = energy + energy_ref[...]
    power = jnp.sum(power_ref[...], axis=1, keepdims=True)
    score_ref[...] = intersection / (
        math.sqrt(coef) * jnp.sqrt((energy / coef + EPS) * (power / coef + EPS))
    )


def final_kernel(coef, half, *refs):
    own_ref, *came, bottom_ref, out_ref, ratio = refs
    tiles = -(-coef // LANES)
    total = own_ref[0]
    for came_ref in came:
        total = total + came_ref[0].astype(f32)
    bottom = bottom_ref[...]
    ratio[0:half, :] = total[0:half] / bottom[0:half]
    ratio[half : 2 * half, :] = total[half : 2 * half] / bottom[0:half]
    for t in range(tiles):
        width = min(LANES, coef - t * LANES)
        pair = ratio[pl.ds(t, 2, stride=half), :]
        out_ref[0, :, pl.ds(t * LANES, width)] = pair[:, :width]


def limit(*arrays):
    size = sum(math.prod(a.shape) * max(2, jnp.dtype(a.dtype).itemsize) for a in arrays)
    return pltpu.CompilerParams(vmem_limit_bytes=(4 << 20) + size)


def body(particles, references, assignment, orientation, tilt_range):
    part_rows = particles.shape[0]
    coef = particles.shape[2]
    owned = references.shape[0]
    devices = lax.axis_size("dom")
    chips = devices // 2
    classes = owned * devices
    assert owned == 1 and classes <= 256 and chips % 8 == 0 and chips & (chips - 1) == 0 and 2 * part_rows <= LANES
    tiles = -(-coef // LANES)
    half = -(-tiles // 4) * 4
    room = 2 * half
    rows = room + 1
    padded = tiles * LANES
    wide = padded + LANES
    shape = jax.ShapeDtypeStruct
    vmem = pl.BlockSpec(memory_space=VMEM)
    hbm = pl.BlockSpec(memory_space=pltpu.HBM)

    nears = chips // FAR

    def hops(step):
        return [(d, d ^ step) for d in range(devices)]

    outs = (
        shape((1, 2, wide), bf16),
        shape((chips * rows, LANES), f32),
        shape((chips * rows, LANES), f32),
        shape((4, part_rows), i32),
    )
    operands = (particles, references, assignment.reshape(part_rows), orientation, tilt_range)
    packet, keep, send, labels = pl.pallas_call(
        functools.partial(sums_kernel, coef, chips, rows, half),
        out_shape=outs,
        in_specs=[hbm] * 5,
        out_specs=(vmem,) * 4,
        scratch_shapes=[
            VMEM(particles.shape, bf16),
            VMEM(references.shape, bf16),
            VMEM((part_rows,), i32),
            VMEM((part_rows,), i32),
            VMEM(tilt_range.shape, i32),
            pltpu.SemaphoreType.DMA((4,)),
            pltpu.SemaphoreType.DMA((PIECES,)),
        ],
        compiler_params=limit(*outs, particles),
        name="sums",
    )(*[pltpu.with_memory_space_constraint(a, pltpu.HBM) for a in operands])
    got = lax.ppermute(send, "dom", hops(1))
    pieces = [packet]
    for k in range(1, FAR):
        pieces.append(lax.ppermute(packet, "dom", hops(2 * nears * k)))
    outs = [shape((FAR, room, LANES), f32 if j == 0 else bf16) for j in range(nears)]
    own, *leave = pl.pallas_call(
        functools.partial(core_kernel, rows),
        out_shape=outs,
        in_specs=[vmem] * 2,
        out_specs=[vmem] * nears,
        compiler_params=limit(keep, got, *outs),
        name="core_add",
    )(keep, got)
    came = []
    for j in range(1, nears):
        came.append(lax.ppermute(leave[j - 1], "dom", hops(2 * j)))
    outs = [shape((1, room, LANES), f32 if k == 0 else bf16) for k in range(FAR)]
    own, *leave = pl.pallas_call(
        near_kernel,
        out_shape=outs,
        in_specs=[vmem] * nears,
        out_specs=[vmem] * FAR,
        compiler_params=limit(own, *came, *outs),
        name="near_add",
    )(own, *came)
    came = []
    for k in range(1, FAR):
        came.append(lax.ppermute(leave[k - 1], "dom", hops(2 * nears * k)))
    same = join(pieces)
    outs = (
        shape((2 * part_rows, padded), bf16),
        shape((part_rows, padded), bf16),
        shape((part_rows, LANES), f32),
    )
    weighted, low, power = pl.pallas_call(
        functools.partial(weigh_kernel, coef),
        out_shape=outs,
        in_specs=[vmem] * 2,
        out_specs=(vmem, vmem, vmem),
        compiler_params=limit(*outs, particles),
        cost_estimate=pl.CostEstimate(flops=10**7, bytes_accessed=10**6, transcendentals=0),
        name="weigh",
    )(particles, labels)
    table = pl.pallas_call(
        table_kernel,
        out_shape=shape((3, 8, padded), f32),
        out_specs=vmem,
        compiler_params=pltpu.CompilerParams(vmem_limit_bytes=4 << 20),
        name="table",
    )()
    pieces = [same]
    for j in range(1, nears):
        pieces.append(lax.ppermute(same, "dom", hops(2 * j)))
    same = join(pieces)
    other = lax.ppermute(same, "dom", hops(1))

    outs = (shape((part_rows, classes), f32),) * 2
    inter, energy = pl.pallas_call(
        own_kernel,
        out_shape=outs,
        in_specs=[vmem] * 3,
        out_specs=(vmem, vmem),
        compiler_params=limit(same, weighted, low),
        name="own",
    )(same, weighted, low)
    outs = (
        shape((part_rows, classes), f32),
        shape((1, classes), f32),
        shape((-(-tiles // 8) * 8, LANES), f32),
    )
    scores, load, bottom = pl.pallas_call(
        functools.partial(post_kernel, coef),
        out_shape=outs,
        in_specs=[vmem] * 8,
        out_specs=(vmem, vmem, vmem),
        scratch_shapes=[
            VMEM((8, padded), f32),
            VMEM((GROUP, 8), f32),
        ],
        compiler_params=limit(same, other, weighted, low, table, *outs),
        name="post",
    )(same, other, weighted, low, power, table, inter, energy)

    class_means = pl.pallas_call(
        functools.partial(final_kernel, coef, half),
        out_shape=shape((owned, 2, coef), f32),
        in_specs=[vmem] * (FAR + 1),
        out_specs=vmem,
        scratch_shapes=[VMEM((room, LANES), f32)],
        compiler_params=pltpu.CompilerParams(vmem_limit_bytes=4 << 20),
        name="means",
    )(own, *came, bottom)
    return (scores, class_means, load.reshape(classes))


def solution(mesh):
    in_specs = (
        P("dom", None, None),
        P("dom", None, None),
        P("dom", None),
        P("dom"),
        P(None, "dom"),
    )
    out_specs = (P("dom", None), P("dom", None, None), P())
    return jax.shard_map(body, mesh=mesh, in_specs=in_specs, out_specs=out_specs, check_vma=False)
```

```python
import functools
import math

import jax
import jax.numpy as jnp
from jax import lax
from jax.experimental import pallas as pl
from jax.experimental.pallas import tpu as pltpu
from jax.sharding import PartitionSpec as P


GRID = 24
ORIENTS = 36

EPS = 1e-06
GAIN = 6.0
TAU = 0.5
LOG2E = math.log2(math.e)
LANES = 128
STEP = 1024
CHUNK = 512
GROUP = 128
FAR = 4
PIECES = 1
VMEM = pltpu.VMEM
f32 = jnp.float32
bf16 = jnp.bfloat16
i32 = jnp.int32


def iota(shape, axis):
    return lax.broadcasted_iota(i32, shape, axis)


def dot(a, b):
    return jnp.dot(a, b, preferred_element_type=f32)


def dot_nt(a, b):
    return lax.dot_general(a, b, (((1,), (1,)), ((), ())), preferred_element_type=f32)


def freqs(index):
    plane = jnp.floor((index + 0.5) * (1.0 / (GRID * GRID)))
    rest = index - plane * (GRID * GRID)
    col_x = jnp.floor((rest + 0.5) * (1.0 / GRID))
    col_z = rest - col_x * GRID
    half = GRID // 2
    freq_x = jnp.where(col_x < half, col_x, col_x - GRID)
    freq_z = jnp.where(col_z < half, col_z, col_z - GRID)
    return freq_x, plane, freq_z


def wedge_of(freq_x, freq_y, freq_z, sin_a, cos_a, cos_c, sin_c, cos_w):
    along = freq_y * cos_a - freq_x * sin_a
    sq = along * along
    zsq = freq_z * freq_z
    inverse = 1.0 / (sq + (zsq + 1.0))
    power = (cos_c * (sq - zsq) + sin_c * (along * freq_z)) * inverse + cos_w
    return 1.0 / (1.0 + jnp.exp2(power))


def by_lane(values, width):
    lane = iota((1, width), 1)
    row = jnp.zeros((1, width), f32)
    for i, value in enumerate(values):
        row = jnp.where(lane == i, f32(value), row)
    return row


def turns(orient, low_bin, high_bin, width):
    quarter = 0.5 * math.pi
    bin_ = 1.5 * math.pi / 180.0
    wide = 80.0 * math.pi / 180.0
    scale = GAIN * LOG2E
    turn = (
        orient * by_lane([2.0 * math.pi / ORIENTS] * 2, width)
        + low_bin * by_lane([0.0, 0.0, -bin_, -bin_, bin_], width)
        + high_bin * by_lane([0.0, 0.0, bin_, bin_, bin_], width)
        + by_lane([0.0, quarter, quarter, 0.0, quarter + wide], width)
    )
    return jnp.sin(turn) * by_lane([1.0, 1.0, -scale, 2.0 * scale, scale], width)


def to_column(row):
    size = row.shape[1]
    same = iota((size, size), 0) == iota((size, size), 1)
    return jnp.sum(jnp.where(same, row, 0.0), axis=1, keepdims=True)


def weights(coef, padded, read, label_ref):
    parts = label_ref.shape[1]
    turn = turns(*[to_column(label_ref[i : i + 1, :].astype(f32)) for i in (1, 2, 3)], LANES)
    factors = [turn[:, i : i + 1] for i in range(5)]
    out_row, in_row = iota((2 * parts, 2 * parts), 0), iota((2 * parts, 2 * parts), 1)
    wanted = jnp.where(out_row < parts, 2 * out_row, 2 * (out_row - parts) + 1)
    split = (in_row == wanted).astype(bf16)
    for start in range(0, padded, STEP):
        width = min(STEP, padded - start)
        valid = min(STEP, coef - start)
        both = dot(split, read(start, valid))
        if valid < width:
            both = jnp.concatenate([both, jnp.zeros((2 * parts, width - valid), f32)], axis=1)
        index = (iota((1, width), 1) + start).astype(f32)
        wedge = wedge_of(*freqs(index), *factors)
        if valid < width:
            wedge = jnp.where(index < coef, wedge, 0.0)
        yield start, width, wedge, both[:parts], both[parts:]


def sums_kernel(
    coef, chips, rows, half, x_hbm, ref_hbm, cls_hbm, orient_hbm, tilt_hbm,
    packet_ref, keep_ref, send_ref, label_ref,
    x_ref, ref_ref, cls_ref, orient_ref, tilt_ref, in_sems, x_sems,
):
    parts = label_ref.shape[1]
    padded = -(-coef // LANES) * LANES
    pairs = ((cls_hbm, cls_ref), (orient_hbm, orient_ref), (tilt_hbm, tilt_ref), (ref_hbm, ref_ref))
    loads = [pltpu.make_async_copy(a, b, in_sems.at[i]) for i, (a, b) in enumerate(pairs)]
    for copy in loads:
        copy.start()
    pieces = x_sems.shape[0]
    span = -(-coef // (STEP * pieces)) * STEP
    copies = []
    for i in range(pieces):
        cols = pl.ds(i * span, min(span, coef - i * span))
        copies.append(
            pltpu.make_async_copy(x_hbm.at[:, :, cols], x_ref.at[:, :, cols], x_sems.at[i])
        )
        copies[-1].start()
    for copy in loads:
        copy.wait()
    label_ref[0:1, :] = cls_ref[...].reshape(1, parts)
    label_ref[1:2, :] = orient_ref[...].reshape(1, parts)
    label_ref[2:4, :] = tilt_ref[...]
    cls = label_ref[0:1, :]

    def read(start, valid):
        if start % span == 0:
            copies[start // span].wait()
        return x_ref[:, :, start : start + valid].reshape(2 * parts, valid)


    spread = (iota((parts, LANES), 1) % parts == iota((parts, LANES), 0)).astype(bf16)
    repeated = dot(label_ref[...].astype(f32).astype(bf16), spread)
    lane = iota(repeated.shape, 1) // parts
    row = jnp.sum(jnp.where(lane == iota(repeated.shape, 0), repeated, 0.0), axis=0, keepdims=True)
    labels = jnp.where(iota((2, LANES), 0) == 0, row, -1.0)
    packet_ref[0, :, padded - LANES : padded] = jnp.zeros((2, LANES), bf16)
    packet_ref[0, :, 0:coef] = ref_ref[0]
    packet_ref[0, :, padded : padded + LANES] = labels.astype(bf16)

    me = lax.axis_index("dom")
    core, chip = me % 2, me // 2
    nears = chips // FAR
    row = iota((2 * chips, parts), 0)
    place = row % chips
    q = ((place % FAR) ^ (chip // nears)) * nears + ((place // FAR) ^ (chip % nears))
    order = 2 * q + jnp.where(row < chips, core, 1 - core)
    hot = (order == cls).astype(bf16)
    for start, width, wedge, real, imag in weights(coef, padded, read, label_ref):
        tile = start // LANES
        for part, value in enumerate((real, imag)):
            summed = dot(hot, (wedge * value).astype(bf16))
            for j in range(width // LANES):
                for q in range(0, chips, 8):
                    place = pl.ds(q * rows + part * half + tile + j, 8, stride=rows)
                    lanes = slice(j * LANES, (j + 1) * LANES)
                    keep_ref[place, :] = summed[q : q + 8, lanes]
                    send_ref[place, :] = summed[chips + q : chips + q + 8, lanes]


def weigh_kernel(coef, x_ref, label_ref, weighted_ref, low_ref, power_ref):
    parts, padded = low_ref.shape
    total = jnp.zeros(power_ref.shape, f32)

    def read(start, valid):
        return x_ref[:, :, start : start + valid].reshape(2 * parts, valid)

    for start, width, wedge, real, imag in weights(coef, padded, read, label_ref):
        cols = slice(start, start + width)
        low_ref[:, cols] = wedge.astype(bf16)
        energy = wedge * (real * real + imag * imag)
        for j in range(width // LANES):
            total = total + energy[:, j * LANES : (j + 1) * LANES]
        weighted_ref[:parts, cols] = (wedge * real).astype(bf16)
        weighted_ref[parts:, cols] = (wedge * imag).astype(bf16)
    power_ref[...] = total


def core_kernel(rows, keep_ref, got_ref, *outs):
    room = outs[0].shape[1]
    for r in range(len(outs) * FAR):
        place = pl.ds(r * rows, room)
        out_ref = outs[r // FAR]
        out_ref[r % FAR] = (keep_ref[place, :] + got_ref[place, :]).astype(out_ref.dtype)


def near_kernel(*refs):
    own_ref, *came = refs[:-FAR]
    outs = refs[-FAR:]
    for k, out_ref in enumerate(outs):
        total = own_ref[k]
        for came_ref in came:
            total = total + came_ref[k].astype(f32)
        out_ref[0] = total.astype(out_ref.dtype)


def join(pieces):
    size, *rest = pieces[0].shape
    hbm = pl.BlockSpec(memory_space=pl.ANY)
    return pl.pallas_call(
        join_kernel,
        out_shape=jax.ShapeDtypeStruct((size * len(pieces), *rest), pieces[0].dtype),
        in_specs=[hbm] * len(pieces),
        out_specs=hbm,
        scratch_shapes=[pltpu.SemaphoreType.DMA((len(pieces),))],
        compiler_params=pltpu.CompilerParams(vmem_limit_bytes=4 << 20),
        name="join",
    )(*pieces)


def join_kernel(*refs):
    *pieces, out_ref, sems = refs
    size = pieces[0].shape[0]
    copies = [
        pltpu.make_async_copy(piece, out_ref.at[pl.ds(i * size, size)], sems.at[i])
        for i, piece in enumerate(pieces)
    ]
    for copy in copies:
        copy.start()
    for copy in copies:
        copy.wait()


def table_kernel(table_ref):
    for t in range(table_ref.shape[2] // LANES):
        index = (iota((8, LANES), 1) + t * LANES).astype(f32)
        for i, row in enumerate(freqs(index)):
            table_ref[i, :, t * LANES : (t + 1) * LANES] = row


def device_of(place, nears, flip):
    me = lax.axis_index("dom")
    chip = me // 2
    far, near = place % FAR, place // FAR
    return 2 * ((far ^ (chip // nears)) * nears + (near ^ (chip % nears))) + me % 2 * (
        1 - 2 * flip
    ) + flip


def rows_of(pieces, cols):
    block = jnp.concatenate([piece[:, :, cols] for piece in pieces])
    return block.reshape(2 * block.shape[0], block.shape[2])


def match(pieces, weighted_ref, low_ref, flip):
    chips = FAR * len(pieces)
    parts, padded = low_ref.shape
    devices = 2 * chips
    inter = jnp.zeros((2 * parts, devices), f32)
    energy = jnp.zeros((parts, devices), f32)
    for start in range(0, padded, CHUNK):
        width = min(CHUNK, padded - start)
        cols = slice(start, start + width)
        rows = rows_of(pieces, cols)
        inter = inter + dot_nt(weighted_ref[:, cols], rows)
        square = rows.astype(f32) * rows.astype(f32)
        pair = square + pltpu.roll(square, devices - 1, 0)
        energy = energy + dot_nt(low_ref[:, cols], pair.astype(bf16))
    row, column = iota((devices, devices), 0), iota((devices, devices), 1)
    here = device_of(row // 2, chips // FAR, flip) == column
    real = (here & (row % 2 == 0)).astype(f32)
    imag = (here & (row % 2 == 1)).astype(f32)

    def pick(a, b):
        return jnp.dot(a, b, precision=lax.Precision.HIGHEST, preferred_element_type=f32)

    return pick(inter[:parts], real) + pick(inter[parts:], imag), pick(energy, real)


def own_kernel(*refs):
    *same, weighted_ref, low_ref, inter_ref, energy_ref = refs
    inter_ref[...], energy_ref[...] = match(same, weighted_ref, low_ref, 0)


def post_kernel(
    coef, weighted_ref, low_ref, power_ref, table, inter_ref, energy_ref, *refs
):
    *refs, score_ref, load_ref, bottom_ref, squares, listed = refs
    same, other = refs[: len(refs) // 2], refs[len(refs) // 2 :]
    chips = FAR * len(same)
    parts, padded = low_ref.shape
    devices = 2 * chips
    classes = score_ref.shape[1]
    tiles = padded // LANES
    me = lax.axis_index("dom")

    cols = slice(padded, padded + LANES)
    labels = jnp.concatenate([rows_of(half, cols).astype(f32) for half in (same, other)])
    every = labels.shape[0]
    cls = labels[:, :parts]

    class_col = iota((classes, parts), 0).astype(f32)
    tally = jnp.zeros((classes, parts), f32)
    for r in range(0, every, 2):
        tally = tally + jnp.where(cls[r : r + 1] == class_col, 1.0, 0.0)
    tally = jnp.sum(tally, axis=1, keepdims=True)
    diagonal = iota((classes, classes), 0) == iota((classes, classes), 1)
    counts = jnp.sum(jnp.where(diagonal, tally, 0.0), axis=0, keepdims=True)
    load_ref[...] = counts * (classes / (devices * parts))

    chosen = cls == me.astype(f32)
    mask = chosen.astype(bf16)
    before = (iota((parts, parts), 0) < iota((parts, parts), 1)).astype(bf16)
    rank = jnp.where(chosen, dot(mask, before), -1.0).astype(bf16)
    held = dot(mask, jnp.ones((parts, every), bf16))
    earlier, later = iota((every, every), 0), iota((every, every), 1)
    start = jnp.sum(jnp.where(earlier < later, held, 0.0), axis=0, keepdims=True)
    stop = jnp.sum(jnp.where(earlier <= later, held, 0.0), axis=0, keepdims=True)
    count = jnp.sum(jnp.where(chosen, 1.0, 0.0)).astype(i32)
    spread = (iota((parts, LANES), 1) % parts == iota((parts, LANES), 0)).astype(bf16)
    gather = (iota((LANES, 8), 0) // parts == iota((LANES, 8), 1) + 1).astype(bf16)

    squares[...] = jnp.zeros_like(squares)

    def group(g, total):
        slot = iota((GROUP, 1), 0).astype(f32) + (g * GROUP).astype(f32)
        in_row = (slot >= start) & (slot < stop)
        row = in_row.astype(bf16)
        within = slot - jnp.sum(jnp.where(in_row, start, 0.0), axis=1, keepdims=True)
        hit = dot((dot(row, rank) == within).astype(bf16), spread)
        columns = dot((hit * dot(row, labels.astype(bf16))).astype(bf16), gather)
        turn = turns(columns[:, 0:1], columns[:, 1:2], columns[:, 2:3], 8)
        empty = iota((GROUP, 8), 0) + g * GROUP >= count
        listed[...] = jnp.where(empty & (iota((GROUP, 8), 1) == 4), 100.0, turn)
        left = jnp.minimum(count - g * GROUP, GROUP)

        def eight(e, total):
            params = listed[pl.ds(pl.multiple_of(e * 8, 8), 8), :]
            factors = [jnp.broadcast_to(params[:, i : i + 1], (8, LANES)) for i in range(5)]
            for t in range(tiles):
                cols = slice(t * LANES, (t + 1) * LANES)
                wedge = wedge_of(table[0, :, cols], table[1, :, cols], table[2, :, cols], *factors)
                squares[:, cols] += (wedge * wedge).astype(bf16).astype(f32)
                if (t + 1) * LANES > coef:
                    wedge = jnp.where(iota((8, LANES), 1) < coef - t * LANES, wedge, 0.0)
                total = total + wedge
            return total

        return lax.fori_loop(0, (left + 7) // 8, eight, total)

    total = lax.fori_loop(0, (count + GROUP - 1) // GROUP, group, jnp.zeros((8, LANES), f32))
    extra = TAU * (jnp.sum(total, keepdims=True) * (1.0 / coef) + 1.0)
    for t in range(tiles):
        cols = slice(t * LANES, (t + 1) * LANES)
        bottom_ref[t : t + 1, :] = jnp.sum(squares[:, cols], axis=0, keepdims=True) + extra

    inter, energy = match(other, weighted_ref, low_ref, 1)
    intersection = inter + inter_ref[...]
    energy = energy + energy_ref[...]
    power = jnp.sum(power_ref[...], axis=1, keepdims=True)
    score_ref[...] = intersection / (
        math.sqrt(coef) * jnp.sqrt((energy / coef + EPS) * (power / coef + EPS))
    )


def final_kernel(coef, half, *refs):
    own_ref, *came, bottom_ref, out_ref, ratio = refs
    tiles = -(-coef // LANES)
    total = own_ref[0]
    for came_ref in came:
        total = total + came_ref[0].astype(f32)
    bottom = bottom_ref[...]
    ratio[0:half, :] = total[0:half] / bottom[0:half]
    ratio[half : 2 * half, :] = total[half : 2 * half] / bottom[0:half]
    for t in range(tiles):
        width = min(LANES, coef - t * LANES)
        pair = ratio[pl.ds(t, 2, stride=half), :]
        out_ref[0, :, pl.ds(t * LANES, width)] = pair[:, :width]


def limit(*arrays):
    size = sum(math.prod(a.shape) * max(2, jnp.dtype(a.dtype).itemsize) for a in arrays)
    return pltpu.CompilerParams(vmem_limit_bytes=(4 << 20) + size)


def body(particles, references, assignment, orientation, tilt_range):
    part_rows = particles.shape[0]
    coef = particles.shape[2]
    owned = references.shape[0]
    devices = lax.axis_size("dom")
    chips = devices // 2
    classes = owned * devices
    assert owned == 1 and classes <= 256 and chips % 8 == 0 and chips & (chips - 1) == 0 and 2 * part_rows <= LANES
    tiles = -(-coef // LANES)
    half = -(-tiles // 4) * 4
    room = 2 * half
    rows = room + 1
    padded = tiles * LANES
    wide = padded + LANES
    shape = jax.ShapeDtypeStruct
    vmem = pl.BlockSpec(memory_space=VMEM)
    hbm = pl.BlockSpec(memory_space=pltpu.HBM)

    nears = chips // FAR

    def hops(step):
        return [(d, d ^ step) for d in range(devices)]

    outs = (
        shape((1, 2, wide), bf16),
        shape((chips * rows, LANES), f32),
        shape((chips * rows, LANES), f32),
        shape((4, part_rows), i32),
    )
    operands = (particles, references, assignment.reshape(part_rows), orientation, tilt_range)
    packet, keep, send, labels = pl.pallas_call(
        functools.partial(sums_kernel, coef, chips, rows, half),
        out_shape=outs,
        in_specs=[hbm] * 5,
        out_specs=(vmem,) * 4,
        scratch_shapes=[
            VMEM(particles.shape, bf16),
            VMEM(references.shape, bf16),
            VMEM((part_rows,), i32),
            VMEM((part_rows,), i32),
            VMEM(tilt_range.shape, i32),
            pltpu.SemaphoreType.DMA((4,)),
            pltpu.SemaphoreType.DMA((PIECES,)),
        ],
        compiler_params=limit(*outs, particles),
        name="sums",
    )(*[pltpu.with_memory_space_constraint(a, pltpu.HBM) for a in operands])
    got = lax.ppermute(send, "dom", hops(1))
    pieces = [packet]
    for k in range(1, FAR):
        pieces.append(lax.ppermute(packet, "dom", hops(2 * nears * k)))
    outs = [shape((FAR, room, LANES), f32 if j == 0 else bf16) for j in range(nears)]
    own, *leave = pl.pallas_call(
        functools.partial(core_kernel, rows),
        out_shape=outs,
        in_specs=[vmem] * 2,
        out_specs=[vmem] * nears,
        compiler_params=limit(keep, got, *outs),
        name="core_add",
    )(keep, got)
    came = []
    for j in range(1, nears):
        came.append(lax.ppermute(leave[j - 1], "dom", hops(2 * j)))
    outs = [shape((1, room, LANES), f32 if k == 0 else bf16) for k in range(FAR)]
    own, *leave = pl.pallas_call(
        near_kernel,
        out_shape=outs,
        in_specs=[vmem] * nears,
        out_specs=[vmem] * FAR,
        compiler_params=limit(own, *came, *outs),
        name="near_add",
    )(own, *came)
    came = []
    for k in range(1, FAR):
        came.append(lax.ppermute(leave[k - 1], "dom", hops(2 * nears * k)))
    same = join(pieces)
    outs = (
        shape((2 * part_rows, padded), bf16),
        shape((part_rows, padded), bf16),
        shape((part_rows, LANES), f32),
    )
    weighted, low, power = pl.pallas_call(
        functools.partial(weigh_kernel, coef),
        out_shape=outs,
        in_specs=[vmem] * 2,
        out_specs=(vmem, vmem, vmem),
        compiler_params=limit(*outs, particles),
        cost_estimate=pl.CostEstimate(flops=10**7, bytes_accessed=10**6, transcendentals=0),
        name="weigh",
    )(particles, labels)
    table = pl.pallas_call(
        table_kernel,
        out_shape=shape((3, 8, padded), f32),
        out_specs=vmem,
        compiler_params=pltpu.CompilerParams(vmem_limit_bytes=4 << 20),
        name="table",
    )()
    pieces = [same]
    for j in range(1, nears):
        pieces.append(lax.ppermute(same, "dom", hops(2 * j)))
    other = []
    for j in range(nears):
        other.append(lax.ppermute(pieces[j], "dom", hops(1)))

    outs = (shape((part_rows, classes), f32),) * 2
    inter, energy = pl.pallas_call(
        own_kernel,
        out_shape=outs,
        in_specs=[vmem] * (nears + 2),
        out_specs=(vmem, vmem),
        compiler_params=limit(*pieces, weighted, low),
        name="own",
    )(*pieces, weighted, low)
    outs = (
        shape((part_rows, classes), f32),
        shape((1, classes), f32),
        shape((-(-tiles // 8) * 8, LANES), f32),
    )
    scores, load, bottom = pl.pallas_call(
        functools.partial(post_kernel, coef),
        out_shape=outs,
        in_specs=[vmem] * (6 + 2 * nears),
        out_specs=(vmem, vmem, vmem),
        scratch_shapes=[
            VMEM((8, padded), f32),
            VMEM((GROUP, 8), f32),
        ],
        compiler_params=limit(*pieces, *other, weighted, low, table, *outs),
        name="post",
    )(weighted, low, power, table, inter, energy, *pieces, *other)

    class_means = pl.pallas_call(
        functools.partial(final_kernel, coef, half),
        out_shape=shape((owned, 2, coef), f32),
        in_specs=[vmem] * (FAR + 1),
        out_specs=vmem,
        scratch_shapes=[VMEM((room, LANES), f32)],
        compiler_params=pltpu.CompilerParams(vmem_limit_bytes=4 << 20),
        name="means",
    )(own, *came, bottom)
    return (scores, class_means, load.reshape(classes))


def solution(mesh):
    in_specs = (
        P("dom", None, None),
        P("dom", None, None),
        P("dom", None),
        P("dom"),
        P(None, "dom"),
    )
    out_specs = (P("dom", None), P("dom", None, None), P())
    return jax.shard_map(body, mesh=mesh, in_specs=in_specs, out_specs=out_specs, check_vma=False)
```
